1024 devices in a mesh: gx: 32 (over z_hi, y), gy: 32 (over x, z_lo, core).
Axes of the slice: x: 4, y: 8, z: 16 (z_hi: 4, z_lo: 4; z = z_hi * 4 + z_lo), core: 2. Of those that a mesh axis runs over, the one named last changes fastest.
Arguments:
- checkpoint: float32 [16, 256, 4096], P(None, 'gy', 'gx'), may hold values from -6 to 6
- trajectory: float32 [16, 256, 4096], P(None, 'gy', 'gx'), may hold values from -6 to 6
- adjoint_forcing: float32 [16, 256, 4096], P(None, 'gy', 'gx'), may hold values from -6 to 6
- east_diffusion: float32 [16, 256, 4096], P(None, 'gy', 'gx'), may hold values from 0.1 to 1
- north_diffusion: float32 [16, 256, 4096], P(None, 'gy', 'gx'), may hold values from 0.3 to 3
- east_wind: float32 [16, 256, 4096], P(None, 'gy', 'gx'), may hold values from -0.6 to 0.6
- north_wind: float32 [16, 256, 4096], P(None, 'gy', 'gx'), may hold values from -6 to 6, as said below
- level_diffusion: float32 [16], replicated, may hold values from 0.1 to 1
- damping: float32 [16], replicated, may hold values from 0.2 to 2
- source: float32 [16, 256, 4096], P(None, 'gy', 'gx'), may hold values from -4 to 5
- observations: float32 [16, 256, 4096], P(None, 'gy', 'gx'), may hold values from -6 to 6
- observation_weight: float32 [16, 256, 4096], P(None, 'gy', 'gx'), may hold values from 0.1 to 1
- step_index: int32 [1], replicated, may hold values from 0 to 95
Outputs:
- forward_state: float32 [16, 256, 4096], P(None, 'gy', 'gx')
- forward_residual: float32 [16, 256, 4096], P(None, 'gy', 'gx')
- adjoint_state: float32 [16, 256, 4096], P(None, 'gy', 'gx')
The draws below stay inside these ranges and needn't reach their ends.
Inputs may be any that keep to these rules, and one draw needn't show every extreme that they name: At every face the magnitude of north_wind is at most twice north_diffusion.
All inputs are finite; a program needn't handle non-finite values.
Results may differ from the reference program's by a relative error of at most 0.000091.
Values sent between devices are 32-bit elements; how exact they have to be, the bound alone decides.
No kernel may reach another device: no remote copies, remote signals or barrier semaphores. Data moves between devices by JAX's collectives and lax.ppermute only.
A program may use at most 32 MiB of HBM per device.

```python
import math
import jax
import jax.numpy as jnp

LEVELS = 16
OUTER = 2
INNER = 4
DAY_STEPS = 96
NLAT = 256
NLON = 4096


def draw_source(key, part):
    noise = jnp.clip(jax.random.normal(key, (LEVELS, NLAT, NLON), jnp.float32), -4.0, 4.0)
    return noise


def flow_parts(key):
    diffusion_key = jax.random.fold_in(key, 4101)
    speed_key = jax.random.fold_in(key, 4102)
    shape = (LEVELS, NLAT, NLON)
    low_log = math.log(0.3)
    high_log = math.log(3.0)
    speed_ratio = jax.random.uniform(speed_key, shape, jnp.float32, -2.0, 2.0)
    diffusion = jnp.exp(jax.random.uniform(diffusion_key, shape, jnp.float32, low_log, high_log))
    diffusion = jnp.clip(diffusion, 0.3, 3.0)
    speed_ratio = jnp.clip(speed_ratio, -2.0, 2.0)
    return (diffusion, diffusion * speed_ratio)


def draw_north_diffusion(key, part):
    return flow_parts(key)[0]


def draw_north_wind(key, part):
    return flow_parts(key)[1]


def level_of(own_key, shape, shards, low, top_value):
    loudness, own = 1.0, jax.random.fold_in(own_key, 6)
    for position, shards_of in shards:
        heights = jnp.exp(jax.random.uniform(jax.random.fold_in(own, position), (shards_of,), jnp.float32, low / len(shards), top_value / len(shards)))
        loudness = loudness * jnp.repeat(heights, shape[position] // shards_of).reshape([-1 if axis == position else 1 for axis in range(len(shape))])
    return loudness


def scatter_about(stream_key, extent, spread, most, pieces=(), kind=jnp.bfloat16):
    loudness = level_of(stream_key, extent, pieces, -0.22, 0.18) if pieces else 1.0
    values = jax.random.normal(stream_key, extent, jnp.float32) * spread * loudness
    return jnp.minimum(jnp.maximum(values, -most), most).astype(kind)


def setup_inputs(seed: int = 0) -> dict:
    streams_of = jax.random.split(jax.random.key(seed), 14)
    checkpoint = scatter_about(streams_of[0], (LEVELS, NLAT, NLON), 1.0, 6.0, ((1, 32), (2, 32)), jnp.float32)
    trajectory = scatter_about(streams_of[1], (LEVELS, NLAT, NLON), 1.0, 6.0, ((1, 32), (2, 32)), jnp.float32)
    adjoint_forcing = scatter_about(streams_of[2], (LEVELS, NLAT, NLON), 1.0, 6.0, ((1, 32), (2, 32)), jnp.float32)
    east_diffusion = jnp.clip(jnp.exp(math.log(1.0) - 2.3025851 * jax.random.uniform(streams_of[3], (LEVELS, NLAT, NLON), jnp.float32) ** level_of(streams_of[3], (LEVELS, NLAT, NLON), ((1, 32), (2, 32)), -0.2, 0.2)), 0.1, 1.0)
    north_diffusion = draw_north_diffusion(jax.random.fold_in(streams_of[13], 71), 0)
    east_wind = jnp.clip(jax.random.uniform(streams_of[5], (LEVELS, NLAT, NLON), jnp.float32, -0.6, 0.6) * level_of(streams_of[5], (LEVELS, NLAT, NLON), ((1, 32), (2, 32)), -0.4, 0.0), -0.6, 0.6)
    north_wind = draw_north_wind(jax.random.fold_in(streams_of[13], 71), 0)
    level_diffusion = jnp.clip(jnp.exp(jax.random.uniform(streams_of[7], (LEVELS,), jnp.float32, math.log(0.1), math.log(1.0))), 0.1, 1.0)
    damping = jnp.clip(jnp.exp(jax.random.uniform(streams_of[8], (LEVELS,), jnp.float32, math.log(0.2), math.log(2.0))), 0.2, 2.0)
    source = draw_source(jax.random.fold_in(streams_of[13], 71), 0)
    observations = scatter_about(streams_of[10], (LEVELS, NLAT, NLON), 1.0, 6.0, ((1, 32), (2, 32)), jnp.float32)
    observation_weight = jnp.clip(jnp.exp(math.log(1.0) - 2.3025851 * jax.random.uniform(streams_of[11], (LEVELS, NLAT, NLON), jnp.float32) ** level_of(streams_of[11], (LEVELS, NLAT, NLON), ((1, 32), (2, 32)), -0.2, 0.2)), 0.1, 1.0)
    step_index = jax.random.randint(streams_of[12], (1,), 0, DAY_STEPS).astype(jnp.int32)
    return {"checkpoint": checkpoint, "trajectory": trajectory, "adjoint_forcing": adjoint_forcing, "east_diffusion": east_diffusion, "north_diffusion": north_diffusion, "east_wind": east_wind, "north_wind": north_wind, "level_diffusion": level_diffusion, "damping": damping, "source": source, "observations": observations, "observation_weight": observation_weight, "step_index": step_index}


RELAXATION = 0.7


def vertical_part(field, up_coef):
    zero_level = jnp.zeros_like(field[:1])
    padded = jnp.concatenate([zero_level, field, zero_level], axis=0)
    flux = up_coef[:, None, None] * (padded[1:] - padded[:-1])
    return -(flux[1:] - flux[:-1])


def apply_forward(west_east, south_north, field, faces):
    east_coef, east_flow, north_coef, north_flow, up_coef = faces
    flux_east = east_flow * (west_east[..., 1:] + west_east[..., :-1]) * 0.5 - east_coef * (west_east[..., 1:] - west_east[..., :-1])
    flux_north = north_flow * (south_north[:, 1:] + south_north[:, :-1]) * 0.5 - north_coef * (south_north[:, 1:] - south_north[:, :-1])
    return (flux_east[..., 1:] - flux_east[..., :-1]) + (flux_north[:, 1:] - flux_north[:, :-1]) + vertical_part(field, up_coef)


def apply_transposed(west_east, south_north, field, faces):
    east_coef, east_flow, north_coef, north_flow, up_coef = faces
    jump_east = west_east[..., :-1] - west_east[..., 1:]
    lower_east = east_flow * 0.5 + east_coef
    upper_east = east_flow * 0.5 - east_coef
    part_east = jump_east[..., 1:] * lower_east[..., 1:] + jump_east[..., :-1] * upper_east[..., :-1]
    jump_north = south_north[:, :-1] - south_north[:, 1:]
    lower_north = north_flow * 0.5 + north_coef
    upper_north = north_flow * 0.5 - north_coef
    part_north = jump_north[:, 1:] * lower_north[:, 1:] + jump_north[:, :-1] * upper_north[:, :-1]
    return part_east + part_north + vertical_part(field, up_coef)


def diagonal_of(tangent, faces, damping):
    east_coef, east_flow, north_coef, north_flow, up_coef = faces
    total = 1.0 + east_coef[..., 1:] + east_coef[..., :-1] + north_coef[:, 1:] + north_coef[:, :-1]
    total = total + (up_coef[1:] + up_coef[:-1])[:, None, None]
    return total + damping[:, None, None] * (1.0 - tangent * tangent)


def global_faces(east_diffusion, north_diffusion, east_wind, north_wind, level_diffusion):
    levels, lat_rows, lon_cols = east_diffusion.shape
    row_mask = (jnp.arange(lat_rows) < lat_rows - 1).astype(jnp.float32)[None, :, None]
    level_mask = (jnp.arange(levels) < levels - 1).astype(jnp.float32)
    north_masked = north_diffusion * row_mask
    flow_masked = north_wind * row_mask
    zero_row = jnp.zeros_like(north_masked[:, :1])
    east_coef = jnp.concatenate([east_diffusion[..., -1:], east_diffusion], axis=2)
    east_flow = jnp.concatenate([east_wind[..., -1:], east_wind], axis=2)
    north_coef = jnp.concatenate([zero_row, north_masked], axis=1)
    north_flow = jnp.concatenate([zero_row, flow_masked], axis=1)
    up_coef = jnp.concatenate([jnp.zeros_like(level_diffusion[:1]), level_diffusion * level_mask])
    return east_coef, east_flow, north_coef, north_flow, up_coef


def wrap_east(field):
    return jnp.concatenate([field[..., -1:], field, field[..., :1]], axis=2)


def pad_north(field):
    zero_row = jnp.zeros_like(field[:, :1])
    return jnp.concatenate([zero_row, field, zero_row], axis=1)


def reference(checkpoint, trajectory, adjoint_forcing, east_diffusion, north_diffusion, east_wind, north_wind, level_diffusion, damping, source, observations, observation_weight, step_index):
    faces = global_faces(east_diffusion, north_diffusion, east_wind, north_wind, level_diffusion)
    levels, lat_rows, lon_cols = checkpoint.shape
    column = jnp.arange(lon_cols).astype(jnp.float32)
    phase = 2.0 * math.pi * column / lon_cols - 2.0 * math.pi * step_index[0].astype(jnp.float32) / DAY_STEPS
    forcing = source * jnp.cos(phase)[None, None, :]
    damp = damping[:, None, None]

    def operate(field):
        return apply_forward(wrap_east(field), pad_north(field), field, faces)

    def operate_transposed(field):
        return apply_transposed(wrap_east(field), pad_north(field), field, faces)

    state = checkpoint
    for newton_step in range(OUTER):
        tangent = jnp.tanh(state)
        diagonal = diagonal_of(tangent, faces, damping)
        resid = state - checkpoint + operate(state) + damp * tangent - forcing
        delta = -RELAXATION * resid / diagonal
        for inner_step in range(INNER - 1):
            image = delta + operate(delta) + damp * (1.0 - tangent * tangent) * delta
            delta = delta + RELAXATION * (-resid - image) / diagonal
        state = state + delta
    final = state - checkpoint + operate(state) + damp * jnp.tanh(state) - forcing

    tangent_n = jnp.tanh(trajectory)
    diagonal_n = diagonal_of(tangent_n, faces, damping)
    local_n = damp * (1.0 - tangent_n * tangent_n)
    multiplier = jnp.zeros_like(trajectory)
    for newton_step in range(OUTER):
        if newton_step == 0:
            resid = -adjoint_forcing
        else:
            resid = multiplier + operate_transposed(multiplier) + local_n * multiplier - adjoint_forcing
        delta = -RELAXATION * resid / diagonal_n
        for inner_step in range(INNER - 1):
            image = delta + operate_transposed(delta) + local_n * delta
            delta = delta + RELAXATION * (-resid - image) / diagonal_n
        multiplier = multiplier + delta
    adjoint_state = multiplier + observation_weight * (state - observations)
    return state, final, adjoint_state
```

```python
import functools
import math

import jax
import jax.numpy as jnp
from jax import lax
from jax.experimental import pallas as pl
from jax.experimental.pallas import tpu as pltpu
from jax.sharding import PartitionSpec as P

DAY_STEPS = 96
RELAXATION = 0.7
SLOT = 16
FIELDS = 8
C, S, ED, EW, ND, NW, TR, AF = range(8)


def lane_ids():
    return lax.broadcasted_iota(jnp.int32, (8, 128), 1)


def pack_kernel(last_ref, *refs):
    fields = refs[:FIELDS]
    bulk, to_east, to_west, far_north, far_south = refs[FIELDS:]
    levels = fields[0].shape[0]
    lanes = lane_ids()
    row = lax.broadcasted_iota(jnp.int32, (8, 128), 0)
    closed = jnp.where((row == 7) & (last_ref[0] == 1), 0.0, 1.0)
    for level in range(levels):
        east = jnp.zeros((8, 128), jnp.float32)
        west = jnp.zeros((8, 128), jnp.float32)
        for k in range(FIELDS):
            value = fields[k][level]
            if k in (ND, NW):
                value = value * closed
            bulk[k, level] = value
            slot = (lanes >= k * SLOT) & (lanes < (k + 1) * SLOT)
            east = jnp.where(slot, pltpu.roll(value, (k * SLOT + SLOT) % 128, 1), east)
            west = jnp.where(slot, pltpu.roll(value, k * SLOT, 1) if k else value, west)
            if k == C:
                far_south[level : level + 1] = value[0:1]
            if k in (C, ND, NW):
                place = {C: 0, ND: 1, NW: 2}[k] * levels + level
                far_north[place : place + 1] = value[7:8]
        to_east[level] = east
        to_west[level] = west


def solve_kernel(
    level_ref,
    damp_ref,
    cos_ref,
    own,
    south,
    north,
    from_west,
    from_east,
    corner_south,
    corner_north,
    far_south,
    far_north,
    observations,
    weight,
    out_state,
    out_resid,
    out_adjoint,
    check,
    force,
    a_c,
    diag,
    up_e,
    low_w,
    up_n,
    low_s,
    low_e,
    up_w,
    low_n,
    up_s,
    wt,
    ctr,
    g,
    d,
    x,
    aq_a,
    wt_a,
    ctr_a,
    g_a,
    d_a,
    mu,
):
    levels = check.shape[0]
    lanes = lane_ids()
    rows = lax.broadcasted_iota(jnp.int32, (24, 256), 0)

    def unroll_roll(value, shift):
        return value if shift % 128 == 0 else pltpu.roll(value, shift % 128, 1)

    def halo(k, west, east):
        left = unroll_roll(west, 128 - SLOT - k * SLOT)
        right = unroll_roll(east, -k * SLOT)
        return jnp.where(lanes < SLOT, right, jnp.where(lanes >= 128 - SLOT, left, 0.0))

    def gather(k, level):
        tiles = []
        for block, west, east in (
            (south, corner_south.at[0], corner_south.at[1]),
            (own, from_west, from_east),
            (north, corner_north.at[0], corner_north.at[1]),
        ):
            tiles.append(
                jnp.concatenate([block[k, level], halo(k, west[level], east[level])], axis=1)
            )
        return jnp.concatenate(tiles, axis=0)

    def wide(ref, index):
        line = ref[index : index + 1]
        line = jnp.concatenate([line, jnp.zeros_like(line)], axis=1)
        return jnp.broadcast_to(line, (24, 256))

    def to_e(v):
        return pltpu.roll(v, 255, 1)

    def to_w(v):
        return pltpu.roll(v, 1, 1)

    def to_n(v):
        return pltpu.roll(v, 23, 0)

    def to_s(v):
        return pltpu.roll(v, 1, 0)

    def up(level):
        return level_ref[level] if level < levels - 1 else None

    def down(level):
        return level_ref[level - 1] if level > 0 else None

    def pair(level):
        parts = [u for u in (up(level), down(level)) if u is not None]
        return sum(parts[1:], parts[0])

    def with_levels(total, level, below, above):
        if above is not None:
            total = total - up(level) * above
        if below is not None:
            total = total - down(level) * below
        return total

    def forward_sum(level, v, below, above, v_n=None, v_s=None):
        v_n = to_n(v) if v_n is None else v_n
        v_s = to_s(v) if v_s is None else v_s
        total = up_e[level] * to_e(v) - low_w[level] * to_w(v)
        total = total + (up_n[level] * v_n - low_s[level] * v_s)
        return with_levels(total, level, below, above)

    def adjoint_sum(level, v, below, above):
        total = up_w[level] * to_w(v) - low_e[level] * to_e(v)
        total = total + (up_s[level] * to_s(v) - low_n[level] * to_n(v))
        return with_levels(total, level, below, above)

    def sweep(field, body):
        below, here = None, field[0]
        for level in range(levels):
            above = field[level + 1] if level + 1 < levels else None
            body(level, here, below, above)
            below, here = here, above

    for level in range(levels):
        ed = gather(ED, level)
        ew = gather(EW, level) * 0.5
        nd = gather(ND, level)
        nw = gather(NW, level) * 0.5
        far_nd = wide(far_south, levels + level)
        far_nw = wide(far_south, 2 * levels + level) * 0.5
        first = rows == 0
        e_low, e_up, n_low, n_up = ew + ed, ew - ed, nw + nd, nw - nd
        w_low, w_up = to_w(e_low), to_w(e_up)
        s_low = jnp.where(first, far_nw + far_nd, to_s(n_low))
        s_up = jnp.where(first, far_nw - far_nd, to_s(n_up))
        up_e[level] = e_up
        low_e[level] = e_low
        up_w[level] = w_up
        low_w[level] = w_low
        up_n[level] = n_up
        low_n[level] = n_low
        up_s[level] = s_up
        low_s[level] = s_low
        center = (e_low - w_up) + (n_low - s_up) + pair(level)
        a_c[level] = center
        base = ed + to_w(ed) + nd + jnp.where(first, far_nd, to_s(nd)) + (1.0 + pair(level))
        diag[level] = base
        check[level] = gather(C, level)
        force[level] = gather(S, level) * cos_ref[...]
        tangent = jnp.tanh(gather(TR, level))
        local = damp_ref[level] * (1.0 - tangent * tangent)
        weight_a = RELAXATION / (base + local)
        af = gather(AF, level)
        diagonal = 1.0 + center + local
        aq_a[level] = diagonal
        wt_a[level] = weight_a
        ctr_a[level] = 1.0 - weight_a * diagonal
        start = weight_a * af
        g_a[level] = start
        d_a[level] = start

    def newton(level, v, resid, tangent):
        local = damp_ref[level] * (1.0 - tangent * tangent)
        w = RELAXATION / (diag[level] + local)
        wt[level] = w
        ctr[level] = 1.0 - w * (1.0 + a_c[level] + local)
        start = -(w * resid)
        g[level] = start
        d[level] = start

    def first_resid(level, v, below, above):
        tangent = jnp.tanh(v)
        v_s = jnp.where(rows == 0, wide(far_south, level), to_s(v))
        v_n = jnp.where(rows == 23, wide(far_north, level), to_n(v))
        total = forward_sum(level, v, below, above, v_n, v_s)
        resid = total + a_c[level] * v + damp_ref[level] * tangent - force[level]
        newton(level, v, resid, tangent)

    def forward_lin(level, v, below, above):
        total = forward_sum(level, v, below, above)
        d[level] = g[level] + ctr[level] * v - wt[level] * total

    def adjoint_lin(level, v, below, above):
        total = adjoint_sum(level, v, below, above)
        d_a[level] = g_a[level] + ctr_a[level] * v - wt_a[level] * total

    def relax(field, body):
        def step(_, carry):
            sweep(field, body)
            return carry

        lax.fori_loop(0, 3, step, 0)

    sweep(check, first_resid)
    relax(d, forward_lin)

    relax(d_a, adjoint_lin)
    for level in range(levels):
        x[level] = check[level] + d[level]
        mu[level] = d_a[level]

    def second_resid(level, v, below, above):
        tangent = jnp.tanh(v)
        total = forward_sum(level, v, below, above)
        moved = v - check[level]
        resid = moved + total + a_c[level] * v + damp_ref[level] * tangent - force[level]
        newton(level, v, resid, tangent)

    def adjoint_resid(level, v, below, above):
        total = adjoint_sum(level, v, below, above)
        af = g_a[level]
        start = af - wt_a[level] * (total + aq_a[level] * v)
        g_a[level] = start
        d_a[level] = start

    sweep(x, second_resid)
    relax(d, forward_lin)
    sweep(mu, adjoint_resid)
    relax(d_a, adjoint_lin)
    for level in range(levels):
        final = x[level] + d[level]
        x[level] = final
        state = final[8:16, :128]
        out_state[level] = state
        multiplier = mu[level, 8:16, :128] + d_a[level, 8:16, :128]
        out_adjoint[level] = multiplier + weight[level] * (state - observations[level])

    def final_resid(level, v, below, above):
        total = forward_sum(level, v, below, above)
        moved = v - check[level]
        resid = moved + total + a_c[level] * v + damp_ref[level] * jnp.tanh(v) - force[level]
        out_resid[level] = resid[8:16, :128]

    sweep(x, final_resid)


def vmem(count):
    return [pl.BlockSpec(memory_space=pltpu.VMEM) for _ in range(count)]


def shifted(array, axis, by, periodic):
    size = lax.axis_size(axis)
    pairs = [(i, (i + by) % size) for i in range(size) if periodic or 0 <= i + by < size]
    return lax.ppermute(array, axis, pairs)


def per_device(
    checkpoint,
    trajectory,
    adjoint_forcing,
    east_diffusion,
    north_diffusion,
    east_wind,
    north_wind,
    level_diffusion,
    damping,
    source,
    observations,
    observation_weight,
    step_index,
):
    levels, lat_rows, lon_cols = checkpoint.shape
    size_x = lax.axis_size("gx")
    size_y = lax.axis_size("gy")
    lane = jnp.arange(256, dtype=jnp.int32)
    column = lax.axis_index("gx") * lon_cols + lane - jnp.where(lane >= 192, 256, 0)
    column = jnp.remainder(column, lon_cols * size_x).astype(jnp.float32)
    phase = (
        2.0 * math.pi * column / (lon_cols * size_x)
        - 2.0 * math.pi * step_index[0].astype(jnp.float32) / DAY_STEPS
    )
    wave = jnp.cos(phase)[None, :]
    last = (lax.axis_index("gy") == size_y - 1).astype(jnp.int32)[None]
    tile = (levels, lat_rows, lon_cols)
    f32 = jnp.float32
    smem = pl.BlockSpec(memory_space=pltpu.SMEM)
    bulk, to_east, to_west, far_up, far_down = pl.pallas_call(
        pack_kernel,
        in_specs=[smem] + vmem(8),
        out_specs=vmem(5),
        out_shape=[
            jax.ShapeDtypeStruct((FIELDS,) + tile, f32),
            jax.ShapeDtypeStruct(tile, f32),
            jax.ShapeDtypeStruct(tile, f32),
            jax.ShapeDtypeStruct((3 * levels, lon_cols), f32),
            jax.ShapeDtypeStruct((levels, lon_cols), f32),
        ],
    )(
        last,
        checkpoint,
        source,
        east_diffusion,
        east_wind,
        north_diffusion,
        north_wind,
        trajectory,
        adjoint_forcing,
    )
    from_west = shifted(to_east, "gx", 1, True)
    from_east = shifted(to_west, "gx", -1, True)
    south = shifted(bulk, "gy", 1, False)
    north = shifted(bulk, "gy", -1, False)
    far_south = shifted(far_up, "gy", 2, False)
    far_north = shifted(far_down, "gy", -2, False)
    corners = jnp.stack([from_west, from_east])
    corner_south = shifted(corners, "gy", 1, False)
    corner_north = shifted(corners, "gy", -1, False)
    scratch = [pltpu.VMEM((levels, 24, 256), f32) for _ in range(23)]
    return tuple(
        pl.pallas_call(
            solve_kernel,
            in_specs=[smem, smem] + vmem(12),
            out_specs=vmem(3),
            out_shape=[jax.ShapeDtypeStruct(tile, f32)] * 3,
            scratch_shapes=scratch,
            compiler_params=pltpu.CompilerParams(vmem_limit_bytes=40 * 1024 * 1024),
        )(
            level_diffusion,
            damping,
            wave,
            bulk,
            south,
            north,
            from_west,
            from_east,
            corner_south,
            corner_north,
            far_south,
            far_north,
            observations,
            observation_weight,
        )
    )


def solution(mesh):
    spread = P(None, "gy", "gx")
    in_specs = (spread,) * 7 + (P(), P()) + (spread,) * 3 + (P(),)
    return jax.shard_map(
        per_device, mesh=mesh, in_specs=in_specs, out_specs=(spread,) * 3, check_vma=False
    )
```

```python
import functools
import math

import jax
import jax.numpy as jnp
from jax import lax
from jax.experimental import pallas as pl
from jax.experimental.pallas import tpu as pltpu
from jax.sharding import PartitionSpec as P

DAY_STEPS = 96
RELAXATION = 0.7
SLOT = 8
FIELDS = 8
FORWARD = 6
C, S, ED, EW, ND, NW, TR, AF = range(8)


def lane_ids():
    return lax.broadcasted_iota(jnp.int32, (8, 128), 1)


def turned(value, shift):
    return value if shift % 128 == 0 else pltpu.roll(value, shift % 128, 1)


def pack_kernel(last_ref, *refs):
    fields = refs[:FIELDS]
    block, block_a, to_east, to_west, far_north, far_south = refs[FIELDS:]
    levels = fields[0].shape[0]
    half = levels // 2
    lanes = lane_ids()
    row = lax.broadcasted_iota(jnp.int32, (8, 128), 0)
    closed = jnp.where((row == 7) & (last_ref[0] == 1), 0.0, 1.0)
    rim_east = jnp.zeros((8, 128), jnp.float32)
    rim_west = jnp.zeros((8, 128), jnp.float32)
    for place in range(half):
        east = jnp.zeros((8, 128), jnp.float32)
        west = jnp.zeros((8, 128), jnp.float32)
        for level in (place, place + half):
            for k in range(FIELDS):
                value = fields[k][level]
                if k in (ND, NW):
                    value = value * closed
                if k < FORWARD:
                    block[k, level] = value
                else:
                    block_a[k - FORWARD, level] = value
                base = SLOT * k + (64 if level >= half else 0)
                slot = (lanes >= base) & (lanes < base + SLOT)
                east = jnp.where(slot, turned(value, base + SLOT), east)
                west = jnp.where(slot, turned(value, base), west)
                if k == C:
                    far_south[level : level + 1] = value[0:1]
                    rim_west = jnp.where(lanes == level, turned(value, level - SLOT), rim_west)
                if k in (C, ND, NW):
                    row_at = {C: 0, ND: 1, NW: 2}[k] * levels + level
                    far_north[row_at : row_at + 1] = value[7:8]
                if k in (C, ED, EW):
                    lane_at = {C: 0, ED: 1, EW: 2}[k] * levels + level
                    moved = turned(value, lane_at - (127 - SLOT))
                    rim_east = jnp.where(lanes == lane_at, moved, rim_east)
        to_east[place] = east
        to_west[place] = west
    to_east[half] = rim_east
    to_west[half] = rim_west


def corner_kernel(block_in, from_west, from_east, block, rims):
    half = from_west.shape[0] - 1
    rims[0] = from_west[half]
    rims[1] = from_east[half]
    for place in range(half):
        block[FORWARD, place] = from_west[place]
        block[FORWARD, half + place] = from_east[place]


def solve_kernel(
    level_ref,
    damp_ref,
    cos_ref,
    own,
    south,
    north,
    own_a,
    south_a,
    north_a,
    rims,
    far_south,
    far_north,
    observations,
    weight,
    out_state,
    out_resid,
    out_adjoint,
    check,
    force,
    a_c,
    diag,
    up_e,
    low_w,
    up_n,
    low_s,
    low_e,
    up_w,
    low_n,
    up_s,
    wt,
    ctr,
    g,
    d,
    x,
    aq_a,
    wt_a,
    ctr_a,
    g_a,
    d_a,
    mu,
):
    levels = check.shape[0]
    lanes = lane_ids()
    rows = lax.broadcasted_iota(jnp.int32, (24, 256), 0)

    half = levels // 2

    def halo(k, level, west, east):
        base = SLOT * k + (64 if level >= half else 0)
        left = turned(west, 128 - SLOT - base)
        right = turned(east, -base)
        return jnp.where(lanes < SLOT, right, jnp.where(lanes >= 128 - SLOT, left, 0.0))

    def gather(k, level):
        place = level % half
        tiles = []
        for block, block_a in ((south, south_a), (own, own_a), (north, north_a)):
            side = halo(k, level, block[FORWARD, place], block[FORWARD, half + place])
            if block is own:
                if k == C:
                    side = jnp.where(lanes == SLOT, turned(rims[1], SLOT - level), side)
                if k in (C, ED, EW):
                    lane_at = {C: 0, ED: 1, EW: 2}[k] * levels + level
                    moved = turned(rims[0], 127 - SLOT - lane_at)
                    side = jnp.where(lanes == 127 - SLOT, moved, side)
            middle = block[k, level] if k < FORWARD else block_a[k - FORWARD, level]
            tiles.append(jnp.concatenate([middle, side], axis=1))
        return jnp.concatenate(tiles, axis=0)

    def wide(ref, index):
        line = ref[index : index + 1]
        line = jnp.concatenate([line, jnp.zeros_like(line)], axis=1)
        return jnp.broadcast_to(line, (24, 256))

    def to_e(v):
        return pltpu.roll(v, 255, 1)

    def to_w(v):
        return pltpu.roll(v, 1, 1)

    def to_n(v):
        return pltpu.roll(v, 23, 0)

    def to_s(v):
        return pltpu.roll(v, 1, 0)

    def up(level):
        return level_ref[level] if level < levels - 1 else None

    def down(level):
        return level_ref[level - 1] if level > 0 else None

    def pair(level):
        parts = [u for u in (up(level), down(level)) if u is not None]
        return sum(parts[1:], parts[0])

    def with_levels(total, level, below, above):
        if above is not None:
            total = total - up(level) * above
        if below is not None:
            total = total - down(level) * below
        return total

    def forward_sum(level, v, below, above, v_n=None, v_s=None):
        v_n = to_n(v) if v_n is None else v_n
        v_s = to_s(v) if v_s is None else v_s
        total = up_e[level] * to_e(v) - low_w[level] * to_w(v)
        total = total + (up_n[level] * v_n - low_s[level] * v_s)
        return with_levels(total, level, below, above)

    def adjoint_sum(level, v, below, above):
        total = up_w[level] * to_w(v) - low_e[level] * to_e(v)
        total = total + (up_s[level] * to_s(v) - low_n[level] * to_n(v))
        return with_levels(total, level, below, above)

    def sweep(field, body):
        below, here = None, field[0]
        for level in range(levels):
            above = field[level + 1] if level + 1 < levels else None
            body(level, here, below, above)
            below, here = here, above

    for level in range(levels):
        ed = gather(ED, level)
        ew = gather(EW, level) * 0.5
        nd = gather(ND, level)
        nw = gather(NW, level) * 0.5
        far_nd = wide(far_south, levels + level)
        far_nw = wide(far_south, 2 * levels + level) * 0.5
        first = rows == 0
        e_low, e_up, n_low, n_up = ew + ed, ew - ed, nw + nd, nw - nd
        w_low, w_up = to_w(e_low), to_w(e_up)
        s_low = jnp.where(first, far_nw + far_nd, to_s(n_low))
        s_up = jnp.where(first, far_nw - far_nd, to_s(n_up))
        up_e[level] = e_up
        low_e[level] = e_low
        up_w[level] = w_up
        low_w[level] = w_low
        up_n[level] = n_up
        low_n[level] = n_low
        up_s[level] = s_up
        low_s[level] = s_low
        center = (e_low - w_up) + (n_low - s_up) + pair(level)
        a_c[level] = center
        base = ed + to_w(ed) + nd + jnp.where(first, far_nd, to_s(nd)) + (1.0 + pair(level))
        diag[level] = base
        check[level] = gather(C, level)
        force[level] = gather(S, level) * cos_ref[...]
        tangent = jnp.tanh(gather(TR, level))
        local = damp_ref[level] * (1.0 - tangent * tangent)
        weight_a = RELAXATION / (base + local)
        af = gather(AF, level)
        diagonal = 1.0 + center + local
        aq_a[level] = diagonal
        wt_a[level] = weight_a
        ctr_a[level] = 1.0 - weight_a * diagonal
        start = weight_a * af
        g_a[level] = start
        d_a[level] = start

    def newton(level, v, resid, tangent):
        local = damp_ref[level] * (1.0 - tangent * tangent)
        w = RELAXATION / (diag[level] + local)
        wt[level] = w
        ctr[level] = 1.0 - w * (1.0 + a_c[level] + local)
        start = -(w * resid)
        g[level] = start
        d[level] = start

    def first_resid(level, v, below, above):
        tangent = jnp.tanh(v)
        v_s = jnp.where(rows == 0, wide(far_south, level), to_s(v))
        v_n = jnp.where(rows == 23, wide(far_north, level), to_n(v))
        total = forward_sum(level, v, below, above, v_n, v_s)
        resid = total + a_c[level] * v + damp_ref[level] * tangent - force[level]
        newton(level, v, resid, tangent)

    def forward_lin(level, v, below, above):
        total = forward_sum(level, v, below, above)
        d[level] = g[level] + ctr[level] * v - wt[level] * total

    def adjoint_lin(level, v, below, above):
        total = adjoint_sum(level, v, below, above)
        d_a[level] = g_a[level] + ctr_a[level] * v - wt_a[level] * total

    def relax(field, body):
        def step(_, carry):
            sweep(field, body)
            return carry

        lax.fori_loop(0, 3, step, 0)

    sweep(check, first_resid)
    relax(d, forward_lin)

    relax(d_a, adjoint_lin)
    for level in range(levels):
        x[level] = check[level] + d[level]
        mu[level] = d_a[level]

    def second_resid(level, v, below, above):
        tangent = jnp.tanh(v)
        total = forward_sum(level, v, below, above)
        moved = v - check[level]
        resid = moved + total + a_c[level] * v + damp_ref[level] * tangent - force[level]
        newton(level, v, resid, tangent)

    def adjoint_resid(level, v, below, above):
        total = adjoint_sum(level, v, below, above)
        af = g_a[level]
        start = af - wt_a[level] * (total + aq_a[level] * v)
        g_a[level] = start
        d_a[level] = start

    sweep(x, second_resid)
    relax(d, forward_lin)
    sweep(mu, adjoint_resid)
    relax(d_a, adjoint_lin)
    for level in range(levels):
        final = x[level] + d[level]
        x[level] = final
        state = final[8:16, :128]
        out_state[level] = state
        multiplier = mu[level, 8:16, :128] + d_a[level, 8:16, :128]
        out_adjoint[level] = multiplier + weight[level] * (state - observations[level])

    def final_resid(level, v, below, above):
        total = forward_sum(level, v, below, above)
        moved = v - check[level]
        resid = moved + total + a_c[level] * v + damp_ref[level] * jnp.tanh(v) - force[level]
        out_resid[level] = resid[8:16, :128]

    sweep(x, final_resid)


def vmem(count):
    return [pl.BlockSpec(memory_space=pltpu.VMEM) for _ in range(count)]


def shifted(array, axis, by, periodic):
    size = lax.axis_size(axis)
    pairs = [(i, (i + by) % size) for i in range(size) if periodic or 0 <= i + by < size]
    return lax.ppermute(array, axis, pairs)


def per_device(
    checkpoint,
    trajectory,
    adjoint_forcing,
    east_diffusion,
    north_diffusion,
    east_wind,
    north_wind,
    level_diffusion,
    damping,
    source,
    observations,
    observation_weight,
    step_index,
):
    levels, lat_rows, lon_cols = checkpoint.shape
    size_x = lax.axis_size("gx")
    size_y = lax.axis_size("gy")
    lane = jnp.arange(256, dtype=jnp.int32)
    column = lax.axis_index("gx") * lon_cols + lane - jnp.where(lane >= 192, 256, 0)
    column = jnp.remainder(column, lon_cols * size_x).astype(jnp.float32)
    phase = (
        2.0 * math.pi * column / (lon_cols * size_x)
        - 2.0 * math.pi * step_index[0].astype(jnp.float32) / DAY_STEPS
    )
    wave = jnp.cos(phase)[None, :]
    last = (lax.axis_index("gy") == size_y - 1).astype(jnp.int32)[None]
    tile = (levels, lat_rows, lon_cols)
    f32 = jnp.float32
    smem = pl.BlockSpec(memory_space=pltpu.SMEM)
    strip = (levels // 2 + 1, lat_rows, lon_cols)
    block, block_a, to_east, to_west, far_up, far_down = pl.pallas_call(
        pack_kernel,
        in_specs=[smem] + vmem(8),
        out_specs=vmem(6),
        out_shape=[
            pltpu.VMEM((FORWARD + 1,) + tile, f32),
            pltpu.VMEM((FIELDS - FORWARD,) + tile, f32),
            pltpu.VMEM(strip, f32),
            pltpu.VMEM(strip, f32),
            pltpu.VMEM((3 * levels, lon_cols), f32),
            pltpu.VMEM((levels, lon_cols), f32),
        ],
    )(
        last,
        checkpoint,
        source,
        east_diffusion,
        east_wind,
        north_diffusion,
        north_wind,
        trajectory,
        adjoint_forcing,
    )
    from_west = shifted(to_east, "gx", 1, True)
    from_east = shifted(to_west, "gx", -1, True)
    block, rims = pl.pallas_call(
        corner_kernel,
        in_specs=vmem(3),
        out_specs=vmem(2),
        out_shape=[
            pltpu.VMEM((FORWARD + 1,) + tile, f32),
            pltpu.VMEM((2, lat_rows, lon_cols), f32),
        ],
        input_output_aliases={0: 0},
        compiler_params=pltpu.CompilerParams(vmem_limit_bytes=4 * 1024 * 1024),
    )(block, from_west, from_east)
    south = shifted(block, "gy", 1, False)
    north = shifted(block, "gy", -1, False)
    far_south = shifted(far_up, "gy", 2, False)
    far_north = shifted(far_down, "gy", -2, False)
    south_a = shifted(block_a, "gy", 1, False)
    north_a = shifted(block_a, "gy", -1, False)
    scratch = [pltpu.VMEM((levels, 24, 256), f32) for _ in range(23)]
    return tuple(
        pl.pallas_call(
            solve_kernel,
            in_specs=[smem, smem] + vmem(12),
            out_specs=vmem(3),
            out_shape=[jax.ShapeDtypeStruct(tile, f32)] * 3,
            scratch_shapes=scratch,
            compiler_params=pltpu.CompilerParams(vmem_limit_bytes=20 * 1024 * 1024),
        )(
            level_diffusion,
            damping,
            wave,
            block,
            south,
            north,
            block_a,
            south_a,
            north_a,
            rims,
            far_south,
            far_north,
            observations,
            observation_weight,
        )
    )


def solution(mesh):
    spread = P(None, "gy", "gx")
    in_specs = (spread,) * 7 + (P(), P()) + (spread,) * 3 + (P(),)
    return jax.shard_map(
        per_device, mesh=mesh, in_specs=in_specs, out_specs=(spread,) * 3, check_vma=False
    )
```

```python
import math

import jax
import jax.numpy as jnp
from jax import lax
from jax.experimental import pallas as pl
from jax.experimental.pallas import tpu as pltpu
from jax.sharding import PartitionSpec as P

DAY_STEPS = 96
RELAXATION = 0.7
SLOT = 8
FIELDS = 8
C, S, ED, EW, ND, NW, TR, AF = range(8)


def lane_ids():
    return lax.broadcasted_iota(jnp.int32, (8, 128), 1)


def turned(value, shift):
    return value if shift % 128 == 0 else pltpu.roll(value, shift % 128, 1)


def pack_kernel(place_ref, *refs):
    fields = refs[:FIELDS]
    block, strip_odd, strip_even, far_first, far_second = refs[FIELDS:]
    odd_x, far_class, last = place_ref[0] == 1, place_ref[1] == 1, place_ref[2] == 1
    levels = fields[0].shape[0]
    half = levels // 2
    lanes = lane_ids()
    row = lax.broadcasted_iota(jnp.int32, (8, 128), 0)
    closed = jnp.where((row == 7) & last, 0.0, 1.0)
    rim_east = jnp.zeros((8, 128), jnp.float32)
    rim_west = jnp.zeros((8, 128), jnp.float32)
    for place in range(half):
        east = jnp.zeros((8, 128), jnp.float32)
        west = jnp.zeros((8, 128), jnp.float32)
        for level in (place, place + half):
            for k in range(FIELDS):
                value = fields[k][level]
                if k in (ND, NW):
                    value = value * closed
                block[k, level] = value
                base = SLOT * k + (64 if level >= half else 0)
                slot = (lanes >= base) & (lanes < base + SLOT)
                east = jnp.where(slot, turned(value, base + SLOT), east)
                west = jnp.where(slot, turned(value, base), west)
                if k == C:
                    rim_west = jnp.where(lanes == level, turned(value, level - SLOT), rim_west)
                if k in (C, ND, NW):
                    row_at = {C: 0, ND: 1, NW: 2}[k] * levels + level
                    high, low = value[7:8], value[0:1]
                    far_first[row_at : row_at + 1] = jnp.where(far_class, low, high)
                    far_second[row_at : row_at + 1] = jnp.where(far_class, high, low)
                if k in (C, ED, EW):
                    lane_at = {C: 0, ED: 1, EW: 2}[k] * levels + level
                    moved = turned(value, lane_at - (127 - SLOT))
                    rim_east = jnp.where(lanes == lane_at, moved, rim_east)
        strip_odd[place] = jnp.where(odd_x, east, west)
        strip_even[place] = jnp.where(odd_x, west, east)
    strip_odd[half] = jnp.where(odd_x, rim_east, rim_west)
    strip_even[half] = jnp.where(odd_x, rim_west, rim_east)


def corner_kernel(place_ref, block_in, from_odd, from_even, block, rims):
    half = from_odd.shape[0] - 1
    odd_x = place_ref[0] == 1
    for place in range(half):
        block[FIELDS, place] = jnp.where(odd_x, from_even[place], from_odd[place])
        block[FIELDS, half + place] = jnp.where(odd_x, from_odd[place], from_even[place])
    rims[0] = jnp.where(odd_x, from_even[half], from_odd[half])
    rims[1] = jnp.where(odd_x, from_odd[half], from_even[half])


def solve_kernel(
    place_ref,
    level_ref,
    damp_ref,
    cos_ref,
    own,
    from_odd,
    from_even,
    rims,
    far_first,
    far_second,
    observations,
    weight,
    out_state,
    out_resid,
    out_adjoint,
    check,
    force,
    a_c,
    diag,
    up_e,
    low_w,
    up_n,
    low_s,
    low_e,
    up_w,
    low_n,
    up_s,
    wt,
    ctr,
    g,
    d,
    x,
    aq_a,
    wt_a,
    ctr_a,
    g_a,
    d_a,
    mu,
):
    levels = check.shape[0]
    lanes = lane_ids()
    rows = lax.broadcasted_iota(jnp.int32, (24, 256), 0)

    half = levels // 2
    odd_y, far_class = place_ref[3] == 1, place_ref[1] == 1

    def tile_south(k, at):
        return jnp.where(odd_y, from_even[k, at], from_odd[k, at])

    def tile_north(k, at):
        return jnp.where(odd_y, from_odd[k, at], from_even[k, at])

    def tile_own(k, at):
        return own[k, at]

    def far_south(at):
        return jnp.where(far_class, far_first[at : at + 1], far_second[at : at + 1])

    def far_north(at):
        return jnp.where(far_class, far_second[at : at + 1], far_first[at : at + 1])

    def halo(k, level, west, east):
        base = SLOT * k + (64 if level >= half else 0)
        left = turned(west, 128 - SLOT - base)
        right = turned(east, -base)
        return jnp.where(lanes < SLOT, right, jnp.where(lanes >= 128 - SLOT, left, 0.0))

    def gather(k, level):
        place = level % half
        tiles = []
        for tile in (tile_south, tile_own, tile_north):
            side = halo(k, level, tile(FIELDS, place), tile(FIELDS, half + place))
            if tile is tile_own:
                if k == C:
                    side = jnp.where(lanes == SLOT, turned(rims[1], SLOT - level), side)
                if k in (C, ED, EW):
                    lane_at = {C: 0, ED: 1, EW: 2}[k] * levels + level
                    moved = turned(rims[0], 127 - SLOT - lane_at)
                    side = jnp.where(lanes == 127 - SLOT, moved, side)
            tiles.append(jnp.concatenate([tile(k, level), side], axis=1))
        return jnp.concatenate(tiles, axis=0)

    def wide(line):
        line = jnp.concatenate([line, jnp.zeros_like(line)], axis=1)
        return jnp.broadcast_to(line, (24, 256))

    def to_e(v):
        return pltpu.roll(v, 255, 1)

    def to_w(v):
        return pltpu.roll(v, 1, 1)

    def to_n(v):
        return pltpu.roll(v, 23, 0)

    def to_s(v):
        return pltpu.roll(v, 1, 0)

    def up(level):
        return level_ref[level] if level < levels - 1 else None

    def down(level):
        return level_ref[level - 1] if level > 0 else None

    def pair(level):
        parts = [u for u in (up(level), down(level)) if u is not None]
        return sum(parts[1:], parts[0])

    def with_levels(total, level, below, above):
        if above is not None:
            total = total - up(level) * above
        if below is not None:
            total = total - down(level) * below
        return total

    def forward_sum(level, v, below, above, v_n=None, v_s=None):
        v_n = to_n(v) if v_n is None else v_n
        v_s = to_s(v) if v_s is None else v_s
        total = up_e[level] * to_e(v) - low_w[level] * to_w(v)
        total = total + (up_n[level] * v_n - low_s[level] * v_s)
        return with_levels(total, level, below, above)

    def adjoint_sum(level, v, below, above):
        total = up_w[level] * to_w(v) - low_e[level] * to_e(v)
        total = total + (up_s[level] * to_s(v) - low_n[level] * to_n(v))
        return with_levels(total, level, below, above)

    def sweep(field, body):
        below, here = None, field[0]
        for level in range(levels):
            above = field[level + 1] if level + 1 < levels else None
            body(level, here, below, above)
            below, here = here, above

    for level in range(levels):
        ed = gather(ED, level)
        ew = gather(EW, level) * 0.5
        nd = gather(ND, level)
        nw = gather(NW, level) * 0.5
        far_nd = wide(far_south(levels + level))
        far_nw = wide(far_south(2 * levels + level)) * 0.5
        first = rows == 0
        e_low, e_up, n_low, n_up = ew + ed, ew - ed, nw + nd, nw - nd
        w_low, w_up = to_w(e_low), to_w(e_up)
        s_low = jnp.where(first, far_nw + far_nd, to_s(n_low))
        s_up = jnp.where(first, far_nw - far_nd, to_s(n_up))
        up_e[level] = e_up
        low_e[level] = e_low
        up_w[level] = w_up
        low_w[level] = w_low
        up_n[level] = n_up
        low_n[level] = n_low
        up_s[level] = s_up
        low_s[level] = s_low
        center = (e_low - w_up) + (n_low - s_up) + pair(level)
        a_c[level] = center
        base = ed + to_w(ed) + nd + jnp.where(first, far_nd, to_s(nd)) + (1.0 + pair(level))
        diag[level] = base
        check[level] = gather(C, level)
        force[level] = gather(S, level) * cos_ref[...]
        tangent = jnp.tanh(gather(TR, level))
        local = damp_ref[level] * (1.0 - tangent * tangent)
        weight_a = RELAXATION / (base + local)
        af = gather(AF, level)
        diagonal = 1.0 + center + local
        aq_a[level] = diagonal
        wt_a[level] = weight_a
        ctr_a[level] = 1.0 - weight_a * diagonal
        start = weight_a * af
        g_a[level] = start
        d_a[level] = start

    def newton(level, resid, tangent):
        local = damp_ref[level] * (1.0 - tangent * tangent)
        w = RELAXATION / (diag[level] + local)
        wt[level] = w
        ctr[level] = 1.0 - w * (1.0 + a_c[level] + local)
        start = -(w * resid)
        g[level] = start
        d[level] = start

    def first_resid(level, v, below, above):
        tangent = jnp.tanh(v)
        v_s = jnp.where(rows == 0, wide(far_south(level)), to_s(v))
        v_n = jnp.where(rows == 23, wide(far_north(level)), to_n(v))
        total = forward_sum(level, v, below, above, v_n, v_s)
        resid = total + a_c[level] * v + damp_ref[level] * tangent - force[level]
        newton(level, resid, tangent)

    def forward_lin(level, v, below, above):
        total = forward_sum(level, v, below, above)
        d[level] = g[level] + ctr[level] * v - wt[level] * total

    def adjoint_lin(level, v, below, above):
        total = adjoint_sum(level, v, below, above)
        d_a[level] = g_a[level] + ctr_a[level] * v - wt_a[level] * total

    def relax(field, body):
        def step(_, carry):
            sweep(field, body)
            return carry

        lax.fori_loop(0, 3, step, 0)

    sweep(check, first_resid)
    relax(d, forward_lin)

    relax(d_a, adjoint_lin)
    for level in range(levels):
        x[level] = check[level] + d[level]
        mu[level] = d_a[level]

    def second_resid(level, v, below, above):
        tangent = jnp.tanh(v)
        total = forward_sum(level, v, below, above)
        moved = v - check[level]
        resid = moved + total + a_c[level] * v + damp_ref[level] * tangent - force[level]
        newton(level, resid, tangent)

    def adjoint_resid(level, v, below, above):
        total = adjoint_sum(level, v, below, above)
        af = g_a[level]
        start = af - wt_a[level] * (total + aq_a[level] * v)
        g_a[level] = start
        d_a[level] = start

    sweep(x, second_resid)
    relax(d, forward_lin)
    sweep(mu, adjoint_resid)
    relax(d_a, adjoint_lin)
    for level in range(levels):
        final = x[level] + d[level]
        x[level] = final
        state = final[8:16, :128]
        out_state[level] = state
        multiplier = mu[level, 8:16, :128] + d_a[level, 8:16, :128]
        out_adjoint[level] = multiplier + weight[level] * (state - observations[level])

    def final_resid(level, v, below, above):
        total = forward_sum(level, v, below, above)
        moved = v - check[level]
        resid = moved + total + a_c[level] * v + damp_ref[level] * jnp.tanh(v) - force[level]
        out_resid[level] = resid[8:16, :128]

    sweep(x, final_resid)


def vmem(count):
    return [pl.BlockSpec(memory_space=pltpu.VMEM) for _ in range(count)]


def swap(array, axis, start, step, periodic):
    size = lax.axis_size(axis)
    pairs = []
    for low in range(size):
        high = low + step
        if (low - start) % (2 * step) < step and (periodic or high < size):
            pairs += [(low, high % size), (high % size, low)]
    return lax.ppermute(array, axis, pairs)


def compute(
    checkpoint,
    trajectory,
    adjoint_forcing,
    east_diffusion,
    north_diffusion,
    east_wind,
    north_wind,
    level_diffusion,
    damping,
    source,
    observations,
    observation_weight,
    step_index,
):
    levels, lat_rows, lon_cols = checkpoint.shape
    size_x = lax.axis_size("gx")
    size_y = lax.axis_size("gy")
    lane = jnp.arange(256, dtype=jnp.int32)
    column = lax.axis_index("gx") * lon_cols + lane - jnp.where(lane >= 192, 256, 0)
    column = jnp.remainder(column, lon_cols * size_x).astype(jnp.float32)
    phase = (
        2.0 * math.pi * column / (lon_cols * size_x)
        - 2.0 * math.pi * step_index[0].astype(jnp.float32) / DAY_STEPS
    )
    wave = jnp.cos(phase)[None, :]
    index_x, index_y = lax.axis_index("gx"), lax.axis_index("gy")
    places = jnp.stack(
        [index_x % 2, index_y // 2 % 2, index_y // (size_y - 1), index_y % 2]
    ).astype(jnp.int32)
    tile = (levels, lat_rows, lon_cols)
    f32 = jnp.float32
    smem = pl.BlockSpec(memory_space=pltpu.SMEM)
    strip = (levels // 2 + 1, lat_rows, lon_cols)
    block, strip_odd, strip_even, far_a, far_b = pl.pallas_call(
        pack_kernel,
        in_specs=[smem] + vmem(8),
        out_specs=vmem(5),
        out_shape=[
            pltpu.VMEM((FIELDS + 1,) + tile, f32),
            pltpu.VMEM(strip, f32),
            pltpu.VMEM(strip, f32),
            pltpu.VMEM((3 * levels, lon_cols), f32),
            pltpu.VMEM((3 * levels, lon_cols), f32),
        ],
    )(
        places,
        checkpoint,
        source,
        east_diffusion,
        east_wind,
        north_diffusion,
        north_wind,
        trajectory,
        adjoint_forcing,
    )
    lon_odd = swap(strip_odd, "gx", 1, 1, True)
    lon_even = swap(strip_even, "gx", 0, 1, True)
    far_first = swap(far_a, "gy", 0, 2, False)
    far_second = swap(far_b, "gy", 2, 2, False)
    block, rims = pl.pallas_call(
        corner_kernel,
        in_specs=[smem] + vmem(3),
        out_specs=vmem(2),
        out_shape=[
            pltpu.VMEM((FIELDS + 1,) + tile, f32),
            pltpu.VMEM((2, lat_rows, lon_cols), f32),
        ],
        input_output_aliases={1: 0},
        compiler_params=pltpu.CompilerParams(vmem_limit_bytes=4 * 1024 * 1024),
    )(places, block, lon_odd, lon_even)
    from_odd = swap(block, "gy", 1, 1, False)
    from_even = swap(block, "gy", 0, 1, False)
    scratch = [pltpu.VMEM((levels, 24, 256), f32) for _ in range(23)]
    return tuple(
        pl.pallas_call(
            solve_kernel,
            in_specs=[smem, smem, smem] + vmem(9),
            out_specs=vmem(3),
            out_shape=[jax.ShapeDtypeStruct(tile, f32)] * 3,
            scratch_shapes=scratch,
            compiler_params=pltpu.CompilerParams(vmem_limit_bytes=20 * 1024 * 1024),
        )(
            places,
            level_diffusion,
            damping,
            wave,
            block,
            from_odd,
            from_even,
            rims,
            far_first,
            far_second,
            observations,
            observation_weight,
        )
    )


def solution(mesh):
    spread = P(None, "gy", "gx")
    in_specs = (spread,) * 7 + (P(), P()) + (spread,) * 3 + (P(),)
    return jax.shard_map(
        compute, mesh=mesh, in_specs=in_specs, out_specs=(spread,) * 3, check_vma=False
    )
```

```python
import functools
import math

import jax
import jax.numpy as jnp
from jax import lax
from jax.experimental import pallas as pl
from jax.experimental.pallas import tpu as pltpu
from jax.sharding import PartitionSpec as P

DAY_STEPS = 96
RELAXATION = 0.7
SLOT = 8
FIELDS = 8
C, S, ED, EW, ND, NW, TR, AF = range(8)


def lane_ids():
    return lax.broadcasted_iota(jnp.int32, (8, 128), 1)


def turned(value, shift):
    return value if shift % 128 == 0 else pltpu.roll(value, shift % 128, 1)


def pack_kernel(size_y, x_ref, y_ref, *refs):
    fields = refs[:FIELDS]
    block, strip_odd, strip_even, far_first, far_second = refs[FIELDS:]
    odd_x, far_class, last = x_ref[0] % 2 == 1, y_ref[0] // 2 % 2 == 1, y_ref[0] == size_y - 1
    levels = fields[0].shape[0]
    half = levels // 2
    lanes = lane_ids()
    row = lax.broadcasted_iota(jnp.int32, (8, 128), 0)
    closed = jnp.where((row == 7) & last, 0.0, 1.0)
    rim_east = jnp.zeros((8, 128), jnp.float32)
    rim_west = jnp.zeros((8, 128), jnp.float32)
    for place in range(half):
        east = jnp.zeros((8, 128), jnp.float32)
        west = jnp.zeros((8, 128), jnp.float32)
        for level in (place, place + half):
            for k in range(FIELDS):
                value = fields[k][level]
                if k in (ND, NW):
                    value = value * closed
                block[k, level] = value
                base = SLOT * k + (64 if level >= half else 0)
                slot = (lanes >= base) & (lanes < base + SLOT)
                east = jnp.where(slot, turned(value, base + SLOT), east)
                west = jnp.where(slot, turned(value, base), west)
                if k == C:
                    rim_west = jnp.where(lanes == level, turned(value, level - SLOT), rim_west)
                if k in (C, ND, NW):
                    row_at = {C: 0, ND: 1, NW: 2}[k] * levels + level
                    high, low = value[7:8], value[0:1]
                    far_first[row_at : row_at + 1] = jnp.where(far_class, low, high)
                    far_second[row_at : row_at + 1] = jnp.where(far_class, high, low)
                if k in (C, ED, EW):
                    lane_at = {C: 0, ED: 1, EW: 2}[k] * levels + level
                    moved = turned(value, lane_at - (127 - SLOT))
                    rim_east = jnp.where(lanes == lane_at, moved, rim_east)
        strip_odd[place] = jnp.where(odd_x, east, west)
        strip_even[place] = jnp.where(odd_x, west, east)
    strip_odd[half] = jnp.where(odd_x, rim_east, rim_west)
    strip_even[half] = jnp.where(odd_x, rim_west, rim_east)


def corner_kernel(x_ref, from_odd, from_even, corners, rims):
    half = from_odd.shape[0] - 1
    odd_x = x_ref[0] % 2 == 1
    for place in range(half):
        corners[place] = jnp.where(odd_x, from_even[place], from_odd[place])
        corners[half + place] = jnp.where(odd_x, from_odd[place], from_even[place])
    rims[0] = jnp.where(odd_x, from_even[half], from_odd[half])
    rims[1] = jnp.where(odd_x, from_odd[half], from_even[half])


def solve_kernel(
    y_ref,
    level_ref,
    damp_ref,
    cos_ref,
    own,
    from_odd,
    from_even,
    corner_own,
    corner_odd,
    corner_even,
    rims,
    far_first,
    far_second,
    observations,
    weight,
    out_state,
    out_resid,
    out_adjoint,
    check,
    force,
    a_c,
    diag,
    up_e,
    low_w,
    up_n,
    low_s,
    low_e,
    up_w,
    low_n,
    up_s,
    wt,
    ctr,
    g,
    d,
    x,
    aq_a,
    wt_a,
    ctr_a,
    g_a,
    d_a,
    mu,
):
    levels = check.shape[0]
    lanes = lane_ids()
    rows = lax.broadcasted_iota(jnp.int32, (24, 256), 0)

    half = levels // 2
    odd_y, far_class = y_ref[0] % 2 == 1, y_ref[0] // 2 % 2 == 1

    def tile_south(k, at):
        return jnp.where(odd_y, from_even[k, at], from_odd[k, at])

    def tile_north(k, at):
        return jnp.where(odd_y, from_odd[k, at], from_even[k, at])

    def tile_own(k, at):
        return own[k, at]

    def side_south(at):
        return jnp.where(odd_y, corner_even[at], corner_odd[at])

    def side_north(at):
        return jnp.where(odd_y, corner_odd[at], corner_even[at])

    def side_own(at):
        return corner_own[at]

    def far_south(at):
        return jnp.where(far_class, far_first[at : at + 1], far_second[at : at + 1])

    def far_north(at):
        return jnp.where(far_class, far_second[at : at + 1], far_first[at : at + 1])

    def halo(k, level, west, east):
        base = SLOT * k + (64 if level >= half else 0)
        left = turned(west, 128 - SLOT - base)
        right = turned(east, -base)
        return jnp.where(lanes < SLOT, right, jnp.where(lanes >= 128 - SLOT, left, 0.0))

    def gather(k, level):
        place = level % half
        tiles = []
        for tile, strip in (
            (tile_south, side_south),
            (tile_own, side_own),
            (tile_north, side_north),
        ):
            side = halo(k, level, strip(place), strip(half + place))
            if tile is tile_own:
                if k == C:
                    side = jnp.where(lanes == SLOT, turned(rims[1], SLOT - level), side)
                if k in (C, ED, EW):
                    lane_at = {C: 0, ED: 1, EW: 2}[k] * levels + level
                    moved = turned(rims[0], 127 - SLOT - lane_at)
                    side = jnp.where(lanes == 127 - SLOT, moved, side)
            tiles.append(jnp.concatenate([tile(k, level), side], axis=1))
        return jnp.concatenate(tiles, axis=0)

    def wide(line):
        line = jnp.concatenate([line, jnp.zeros_like(line)], axis=1)
        return jnp.broadcast_to(line, (24, 256))

    def to_e(v):
        return pltpu.roll(v, 255, 1)

    def to_w(v):
        return pltpu.roll(v, 1, 1)

    def to_n(v):
        return pltpu.roll(v, 23, 0)

    def to_s(v):
        return pltpu.roll(v, 1, 0)

    def up(level):
        return level_ref[level] if level < levels - 1 else None

    def down(level):
        return level_ref[level - 1] if level > 0 else None

    def pair(level):
        parts = [u for u in (up(level), down(level)) if u is not None]
        return sum(parts[1:], parts[0])

    def with_levels(total, level, below, above):
        if above is not None:
            total = total - up(level) * above
        if below is not None:
            total = total - down(level) * below
        return total

    def forward_sum(level, v, below, above, v_n=None, v_s=None):
        v_n = to_n(v) if v_n is None else v_n
        v_s = to_s(v) if v_s is None else v_s
        total = up_e[level] * to_e(v) - low_w[level] * to_w(v)
        total = total + (up_n[level] * v_n - low_s[level] * v_s)
        return with_levels(total, level, below, above)

    def adjoint_sum(level, v, below, above):
        total = up_w[level] * to_w(v) - low_e[level] * to_e(v)
        total = total + (up_s[level] * to_s(v) - low_n[level] * to_n(v))
        return with_levels(total, level, below, above)

    def sweep(field, body):
        below, here = None, field[0]
        for level in range(levels):
            above = field[level + 1] if level + 1 < levels else None
            body(level, here, below, above)
            below, here = here, above

    for level in range(levels):
        ed = gather(ED, level)
        ew = gather(EW, level) * 0.5
        nd = gather(ND, level)
        nw = gather(NW, level) * 0.5
        far_nd = wide(far_south(levels + level))
        far_nw = wide(far_south(2 * levels + level)) * 0.5
        first = rows == 0
        e_low, e_up, n_low, n_up = ew + ed, ew - ed, nw + nd, nw - nd
        w_low, w_up = to_w(e_low), to_w(e_up)
        s_low = jnp.where(first, far_nw + far_nd, to_s(n_low))
        s_up = jnp.where(first, far_nw - far_nd, to_s(n_up))
        up_e[level] = e_up
        low_e[level] = e_low
        up_w[level] = w_up
        low_w[level] = w_low
        up_n[level] = n_up
        low_n[level] = n_low
        up_s[level] = s_up
        low_s[level] = s_low
        center = (e_low - w_up) + (n_low - s_up) + pair(level)
        a_c[level] = center
        base = ed + to_w(ed) + nd + jnp.where(first, far_nd, to_s(nd)) + (1.0 + pair(level))
        diag[level] = base
        check[level] = gather(C, level)
        force[level] = gather(S, level) * cos_ref[...]
        tangent = jnp.tanh(gather(TR, level))
        local = damp_ref[level] * (1.0 - tangent * tangent)
        weight_a = RELAXATION / (base + local)
        af = gather(AF, level)
        diagonal = 1.0 + center + local
        aq_a[level] = diagonal
        wt_a[level] = weight_a
        ctr_a[level] = 1.0 - weight_a * diagonal
        start = weight_a * af
        g_a[level] = start
        d_a[level] = start

    def newton(level, resid, tangent):
        local = damp_ref[level] * (1.0 - tangent * tangent)
        w = RELAXATION / (diag[level] + local)
        wt[level] = w
        ctr[level] = 1.0 - w * (1.0 + a_c[level] + local)
        start = -(w * resid)
        g[level] = start
        d[level] = start

    def first_resid(level, v, below, above):
        tangent = jnp.tanh(v)
        v_s = jnp.where(rows == 0, wide(far_south(level)), to_s(v))
        v_n = jnp.where(rows == 23, wide(far_north(level)), to_n(v))
        total = forward_sum(level, v, below, above, v_n, v_s)
        resid = total + a_c[level] * v + damp_ref[level] * tangent - force[level]
        newton(level, resid, tangent)

    def forward_lin(level, v, below, above):
        total = forward_sum(level, v, below, above)
        d[level] = g[level] + ctr[level] * v - wt[level] * total

    def adjoint_lin(level, v, below, above):
        total = adjoint_sum(level, v, below, above)
        d_a[level] = g_a[level] + ctr_a[level] * v - wt_a[level] * total

    def relax(field, body):
        def step(_, carry):
            sweep(field, body)
            return carry

        lax.fori_loop(0, 3, step, 0)

    sweep(check, first_resid)
    relax(d, forward_lin)

    relax(d_a, adjoint_lin)
    for level in range(levels):
        x[level] = check[level] + d[level]
        mu[level] = d_a[level]

    def second_resid(level, v, below, above):
        tangent = jnp.tanh(v)
        total = forward_sum(level, v, below, above)
        moved = v - check[level]
        resid = moved + total + a_c[level] * v + damp_ref[level] * tangent - force[level]
        newton(level, resid, tangent)

    def adjoint_resid(level, v, below, above):
        total = adjoint_sum(level, v, below, above)
        af = g_a[level]
        start = af - wt_a[level] * (total + aq_a[level] * v)
        g_a[level] = start
        d_a[level] = start

    sweep(x, second_resid)
    relax(d, forward_lin)
    sweep(mu, adjoint_resid)
    relax(d_a, adjoint_lin)
    for level in range(levels):
        final = x[level] + d[level]
        x[level] = final
        state = final[8:16, :128]
        out_state[level] = state
        multiplier = mu[level, 8:16, :128] + d_a[level, 8:16, :128]
        out_adjoint[level] = multiplier + weight[level] * (state - observations[level])

    def final_resid(level, v, below, above):
        total = forward_sum(level, v, below, above)
        moved = v - check[level]
        resid = moved + total + a_c[level] * v + damp_ref[level] * jnp.tanh(v) - force[level]
        out_resid[level] = resid[8:16, :128]

    sweep(x, final_resid)


def vmem(count):
    return [pl.BlockSpec(memory_space=pltpu.VMEM) for _ in range(count)]


def swap(array, axis, start, step, periodic):
    size = lax.axis_size(axis)
    pairs = []
    for low in range(size):
        high = low + step
        if (low - start) % (2 * step) < step and (periodic or high < size):
            pairs += [(low, high % size), (high % size, low)]
    return lax.ppermute(array, axis, pairs)


def compute(
    checkpoint,
    trajectory,
    adjoint_forcing,
    east_diffusion,
    north_diffusion,
    east_wind,
    north_wind,
    level_diffusion,
    damping,
    source,
    observations,
    observation_weight,
    step_index,
):
    levels, lat_rows, lon_cols = checkpoint.shape
    size_x = lax.axis_size("gx")
    size_y = lax.axis_size("gy")
    lane = jnp.arange(256, dtype=jnp.int32)
    column = lax.axis_index("gx") * lon_cols + lane - jnp.where(lane >= 192, 256, 0)
    column = jnp.remainder(column, lon_cols * size_x).astype(jnp.float32)
    phase = (
        2.0 * math.pi * column / (lon_cols * size_x)
        - 2.0 * math.pi * step_index[0].astype(jnp.float32) / DAY_STEPS
    )
    wave = jnp.cos(phase)[None, :]
    index_x, index_y = lax.axis_index("gx"), lax.axis_index("gy")
    place_x = index_x.astype(jnp.int32)[None]
    place_y = index_y.astype(jnp.int32)[None]
    tile = (levels, lat_rows, lon_cols)
    f32 = jnp.float32
    smem = pl.BlockSpec(memory_space=pltpu.SMEM)
    strip = (levels // 2 + 1, lat_rows, lon_cols)
    block, strip_odd, strip_even, far_a, far_b = pl.pallas_call(
        functools.partial(pack_kernel, size_y),
        in_specs=[smem, smem] + vmem(8),
        out_specs=vmem(5),
        out_shape=[
            pltpu.VMEM((FIELDS,) + tile, f32),
            pltpu.VMEM(strip, f32),
            pltpu.VMEM(strip, f32),
            pltpu.VMEM((3 * levels, lon_cols), f32),
            pltpu.VMEM((3 * levels, lon_cols), f32),
        ],
    )(
        place_x,
        place_y,
        checkpoint,
        source,
        east_diffusion,
        east_wind,
        north_diffusion,
        north_wind,
        trajectory,
        adjoint_forcing,
    )
    from_odd = swap(block, "gy", 1, 1, False)
    from_even = swap(block, "gy", 0, 1, False)
    lon_odd = swap(strip_odd, "gx", 1, 1, True)
    lon_even = swap(strip_even, "gx", 0, 1, True)
    far_first = swap(far_a, "gy", 0, 2, False)
    far_second = swap(far_b, "gy", 2, 2, False)
    corners, rims = pl.pallas_call(
        corner_kernel,
        in_specs=[smem] + vmem(2),
        out_specs=vmem(2),
        out_shape=[
            pltpu.VMEM(tile, f32),
            pltpu.VMEM((2, lat_rows, lon_cols), f32),
        ],
        compiler_params=pltpu.CompilerParams(vmem_limit_bytes=4 * 1024 * 1024),
    )(place_x, lon_odd, lon_even)
    corner_odd = swap(corners, "gy", 1, 1, False)
    corner_even = swap(corners, "gy", 0, 1, False)
    scratch = [pltpu.VMEM((levels, 24, 256), f32) for _ in range(23)]
    return tuple(
        pl.pallas_call(
            solve_kernel,
            in_specs=[smem, smem, smem] + vmem(12),
            out_specs=vmem(3),
            out_shape=[jax.ShapeDtypeStruct(tile, f32)] * 3,
            scratch_shapes=scratch,
            compiler_params=pltpu.CompilerParams(vmem_limit_bytes=20 * 1024 * 1024),
        )(
            place_y,
            level_diffusion,
            damping,
            wave,
            block,
            from_odd,
            from_even,
            corners,
            corner_odd,
            corner_even,
            rims,
            far_first,
            far_second,
            observations,
            observation_weight,
        )
    )


def solution(mesh):
    spread = P(None, "gy", "gx")
    in_specs = (spread,) * 7 + (P(), P()) + (spread,) * 3 + (P(),)
    return jax.shard_map(
        compute, mesh=mesh, in_specs=in_specs, out_specs=(spread,) * 3, check_vma=False
    )
```

```python
import functools
import math

import jax
import jax.numpy as jnp
from jax import lax
from jax.experimental import pallas as pl
from jax.experimental.pallas import tpu as pltpu
from jax.sharding import PartitionSpec as P

DAY_STEPS = 96
RELAXATION = 0.7
SLOT = 8
FIELDS = 8
C, S, ED, EW, ND, NW, TR, AF = range(8)


def lane_ids():
    return lax.broadcasted_iota(jnp.int32, (8, 128), 1)


def turned(value, shift):
    return value if shift % 128 == 0 else pltpu.roll(value, shift % 128, 1)


def pack_kernel(size_y, x_ref, y_ref, *refs):
    fields = refs[:FIELDS]
    block, strip_odd, strip_even = refs[FIELDS:]
    odd_x, last = x_ref[0] % 2 == 1, y_ref[0] == size_y - 1
    levels = fields[0].shape[0]
    half = levels // 2
    lanes = lane_ids()
    row = lax.broadcasted_iota(jnp.int32, (8, 128), 0)
    closed = jnp.where((row == 7) & last, 0.0, 1.0)
    rim_east = jnp.zeros((8, 128), jnp.float32)
    rim_west = jnp.zeros((8, 128), jnp.float32)
    for place in range(half):
        east = jnp.zeros((8, 128), jnp.float32)
        west = jnp.zeros((8, 128), jnp.float32)
        for level in (place, place + half):
            for k in range(FIELDS):
                value = fields[k][level]
                if k in (ND, NW):
                    value = value * closed
                block[k, level] = value
                base = SLOT * k + (64 if level >= half else 0)
                slot = (lanes >= base) & (lanes < base + SLOT)
                east = jnp.where(slot, turned(value, base + SLOT), east)
                west = jnp.where(slot, turned(value, base), west)
                if k == C:
                    rim_west = jnp.where(lanes == level, turned(value, level - SLOT), rim_west)
                if k in (C, ED, EW):
                    lane_at = {C: 0, ED: 1, EW: 2}[k] * levels + level
                    moved = turned(value, lane_at - (127 - SLOT))
                    rim_east = jnp.where(lanes == lane_at, moved, rim_east)
        strip_odd[place] = jnp.where(odd_x, east, west)
        strip_even[place] = jnp.where(odd_x, west, east)
    strip_odd[half] = jnp.where(odd_x, rim_east, rim_west)
    strip_even[half] = jnp.where(odd_x, rim_west, rim_east)


def relay(odd_y, high_when_odd, block, corners):
    levels = block.shape[1]
    for row in range(3 * levels):
        value = block[(C, ND, NW)[row // levels], row % levels]
        high, low = value[7:8], value[0:1]
        line = jnp.where(odd_y, high, low) if high_when_odd else jnp.where(odd_y, low, high)
        at = row % 8
        corners[levels + row // 8, at : at + 1] = line


def corner_odd_kernel(x_ref, y_ref, from_odd, from_even, block_even, corners, rims):
    half = from_odd.shape[0] - 1
    odd_x = x_ref[0] % 2 == 1
    for place in range(half):
        corners[place] = jnp.where(odd_x, from_even[place], from_odd[place])
        corners[half + place] = jnp.where(odd_x, from_odd[place], from_even[place])
    rims[0] = jnp.where(odd_x, from_even[half], from_odd[half])
    rims[1] = jnp.where(odd_x, from_odd[half], from_even[half])
    relay(y_ref[0] % 2 == 1, True, block_even, corners)


def corner_even_kernel(y_ref, corner_own, block_odd, corners):
    for place in range(block_odd.shape[1]):
        corners[place] = corner_own[place]
    relay(y_ref[0] % 2 == 1, False, block_odd, corners)


def solve_kernel(
    y_ref,
    level_ref,
    damp_ref,
    cos_ref,
    own,
    from_odd,
    from_even,
    corner_own,
    corner_odd,
    corner_even,
    rims,
    observations,
    weight,
    out_state,
    out_resid,
    out_adjoint,
    check,
    force,
    a_c,
    diag,
    up_e,
    low_w,
    up_n,
    low_s,
    low_e,
    up_w,
    low_n,
    up_s,
    wt,
    ctr,
    g,
    d,
    x,
    aq_a,
    wt_a,
    ctr_a,
    g_a,
    d_a,
    mu,
):
    levels = check.shape[0]
    lanes = lane_ids()
    rows = lax.broadcasted_iota(jnp.int32, (24, 256), 0)

    half = levels // 2
    odd_y = y_ref[0] % 2 == 1

    def tile_south(k, at):
        return jnp.where(odd_y, from_even[k, at], from_odd[k, at])

    def tile_north(k, at):
        return jnp.where(odd_y, from_odd[k, at], from_even[k, at])

    def tile_own(k, at):
        return own[k, at]

    def side_south(at):
        return jnp.where(odd_y, corner_even[at], corner_odd[at])

    def side_north(at):
        return jnp.where(odd_y, corner_odd[at], corner_even[at])

    def side_own(at):
        return corner_own[at]

    def far_south(at):
        tile, row = levels + at // 8, at % 8
        return side_south(tile)[row : row + 1]

    def far_north(at):
        tile, row = levels + at // 8, at % 8
        return side_north(tile)[row : row + 1]

    def halo(k, level, west, east):
        base = SLOT * k + (64 if level >= half else 0)
        left = turned(west, 128 - SLOT - base)
        right = turned(east, -base)
        return jnp.where(lanes < SLOT, right, jnp.where(lanes >= 128 - SLOT, left, 0.0))

    def gather(k, level):
        place = level % half
        tiles = []
        for tile, strip in (
            (tile_south, side_south),
            (tile_own, side_own),
            (tile_north, side_north),
        ):
            side = halo(k, level, strip(place), strip(half + place))
            if tile is tile_own:
                if k == C:
                    side = jnp.where(lanes == SLOT, turned(rims[1], SLOT - level), side)
                if k in (C, ED, EW):
                    lane_at = {C: 0, ED: 1, EW: 2}[k] * levels + level
                    moved = turned(rims[0], 127 - SLOT - lane_at)
                    side = jnp.where(lanes == 127 - SLOT, moved, side)
            tiles.append(jnp.concatenate([tile(k, level), side], axis=1))
        return jnp.concatenate(tiles, axis=0)

    def wide(line):
        line = jnp.concatenate([line, jnp.zeros_like(line)], axis=1)
        return jnp.broadcast_to(line, (24, 256))

    def to_e(v):
        return pltpu.roll(v, 255, 1)

    def to_w(v):
        return pltpu.roll(v, 1, 1)

    def to_n(v):
        return pltpu.roll(v, 23, 0)

    def to_s(v):
        return pltpu.roll(v, 1, 0)

    def up(level):
        return level_ref[level] if level < levels - 1 else None

    def down(level):
        return level_ref[level - 1] if level > 0 else None

    def pair(level):
        parts = [u for u in (up(level), down(level)) if u is not None]
        return sum(parts[1:], parts[0])

    def with_levels(total, level, below, above):
        if above is not None:
            total = total - up(level) * above
        if below is not None:
            total = total - down(level) * below
        return total

    def forward_sum(level, v, below, above, v_n=None, v_s=None):
        v_n = to_n(v) if v_n is None else v_n
        v_s = to_s(v) if v_s is None else v_s
        total = up_e[level] * to_e(v) - low_w[level] * to_w(v)
        total = total + (up_n[level] * v_n - low_s[level] * v_s)
        return with_levels(total, level, below, above)

    def adjoint_sum(level, v, below, above):
        total = up_w[level] * to_w(v) - low_e[level] * to_e(v)
        total = total + (up_s[level] * to_s(v) - low_n[level] * to_n(v))
        return with_levels(total, level, below, above)

    def sweep(field, body):
        below, here = None, field[0]
        for level in range(levels):
            above = field[level + 1] if level + 1 < levels else None
            body(level, here, below, above)
            below, here = here, above

    for level in range(levels):
        ed = gather(ED, level)
        ew = gather(EW, level) * 0.5
        nd = gather(ND, level)
        nw = gather(NW, level) * 0.5
        far_nd = wide(far_south(levels + level))
        far_nw = wide(far_south(2 * levels + level)) * 0.5
        first = rows == 0
        e_low, e_up, n_low, n_up = ew + ed, ew - ed, nw + nd, nw - nd
        w_low, w_up = to_w(e_low), to_w(e_up)
        s_low = jnp.where(first, far_nw + far_nd, to_s(n_low))
        s_up = jnp.where(first, far_nw - far_nd, to_s(n_up))
        up_e[level] = e_up
        low_e[level] = e_low
        up_w[level] = w_up
        low_w[level] = w_low
        up_n[level] = n_up
        low_n[level] = n_low
        up_s[level] = s_up
        low_s[level] = s_low
        center = (e_low - w_up) + (n_low - s_up) + pair(level)
        a_c[level] = center
        base = ed + to_w(ed) + nd + jnp.where(first, far_nd, to_s(nd)) + (1.0 + pair(level))
        diag[level] = base
        check[level] = gather(C, level)
        force[level] = gather(S, level) * cos_ref[...]
        tangent = jnp.tanh(gather(TR, level))
        local = damp_ref[level] * (1.0 - tangent * tangent)
        weight_a = RELAXATION / (base + local)
        af = gather(AF, level)
        diagonal = 1.0 + center + local
        aq_a[level] = diagonal
        wt_a[level] = weight_a
        ctr_a[level] = 1.0 - weight_a * diagonal
        start = weight_a * af
        g_a[level] = start
        d_a[level] = start

    def newton(level, resid, tangent):
        local = damp_ref[level] * (1.0 - tangent * tangent)
        w = RELAXATION / (diag[level] + local)
        wt[level] = w
        ctr[level] = 1.0 - w * (1.0 + a_c[level] + local)
        start = -(w * resid)
        g[level] = start
        d[level] = start

    def first_resid(level, v, below, above):
        tangent = jnp.tanh(v)
        v_s = jnp.where(rows == 0, wide(far_south(level)), to_s(v))
        v_n = jnp.where(rows == 23, wide(far_north(level)), to_n(v))
        total = forward_sum(level, v, below, above, v_n, v_s)
        resid = total + a_c[level] * v + damp_ref[level] * tangent - force[level]
        newton(level, resid, tangent)

    def forward_lin(level, v, below, above):
        total = forward_sum(level, v, below, above)
        d[level] = g[level] + ctr[level] * v - wt[level] * total

    def adjoint_lin(level, v, below, above):
        total = adjoint_sum(level, v, below, above)
        d_a[level] = g_a[level] + ctr_a[level] * v - wt_a[level] * total

    def relax(field, body):
        def step(_, carry):
            sweep(field, body)
            return carry

        lax.fori_loop(0, 3, step, 0)

    sweep(check, first_resid)
    relax(d, forward_lin)

    relax(d_a, adjoint_lin)
    for level in range(levels):
        x[level] = check[level] + d[level]
        mu[level] = d_a[level]

    def second_resid(level, v, below, above):
        tangent = jnp.tanh(v)
        total = forward_sum(level, v, below, above)
        moved = v - check[level]
        resid = moved + total + a_c[level] * v + damp_ref[level] * tangent - force[level]
        newton(level, resid, tangent)

    def adjoint_resid(level, v, below, above):
        total = adjoint_sum(level, v, below, above)
        af = g_a[level]
        start = af - wt_a[level] * (total + aq_a[level] * v)
        g_a[level] = start
        d_a[level] = start

    sweep(x, second_resid)
    relax(d, forward_lin)
    sweep(mu, adjoint_resid)
    relax(d_a, adjoint_lin)
    for level in range(levels):
        final = x[level] + d[level]
        x[level] = final
        state = final[8:16, :128]
        out_state[level] = state
        multiplier = mu[level, 8:16, :128] + d_a[level, 8:16, :128]
        out_adjoint[level] = multiplier + weight[level] * (state - observations[level])

    def final_resid(level, v, below, above):
        total = forward_sum(level, v, below, above)
        moved = v - check[level]
        resid = moved + total + a_c[level] * v + damp_ref[level] * jnp.tanh(v) - force[level]
        out_resid[level] = resid[8:16, :128]

    sweep(x, final_resid)


def vmem(count):
    return [pl.BlockSpec(memory_space=pltpu.VMEM) for _ in range(count)]


def swap(array, axis, start, step, periodic):
    size = lax.axis_size(axis)
    pairs = []
    for low in range(size):
        high = low + step
        if (low - start) % (2 * step) < step and (periodic or high < size):
            pairs += [(low, high % size), (high % size, low)]
    return lax.ppermute(array, axis, pairs)


def compute(
    checkpoint,
    trajectory,
    adjoint_forcing,
    east_diffusion,
    north_diffusion,
    east_wind,
    north_wind,
    level_diffusion,
    damping,
    source,
    observations,
    observation_weight,
    step_index,
):
    levels, lat_rows, lon_cols = checkpoint.shape
    size_x = lax.axis_size("gx")
    size_y = lax.axis_size("gy")
    lane = jnp.arange(256, dtype=jnp.int32)
    column = lax.axis_index("gx") * lon_cols + lane - jnp.where(lane >= 192, 256, 0)
    column = jnp.remainder(column, lon_cols * size_x).astype(jnp.float32)
    phase = (
        2.0 * math.pi * column / (lon_cols * size_x)
        - 2.0 * math.pi * step_index[0].astype(jnp.float32) / DAY_STEPS
    )
    wave = jnp.cos(phase)[None, :]
    index_x, index_y = lax.axis_index("gx"), lax.axis_index("gy")
    place_x = index_x.astype(jnp.int32)[None]
    place_y = index_y.astype(jnp.int32)[None]
    tile = (levels, lat_rows, lon_cols)
    f32 = jnp.float32
    smem = pl.BlockSpec(memory_space=pltpu.SMEM)
    strip = (levels // 2 + 1, lat_rows, lon_cols)
    block, strip_odd, strip_even = pl.pallas_call(
        functools.partial(pack_kernel, size_y),
        in_specs=[smem, smem] + vmem(8),
        out_specs=vmem(3),
        out_shape=[
            pltpu.VMEM((FIELDS,) + tile, f32),
            pltpu.VMEM(strip, f32),
            pltpu.VMEM(strip, f32),
        ],
    )(
        place_x,
        place_y,
        checkpoint,
        source,
        east_diffusion,
        east_wind,
        north_diffusion,
        north_wind,
        trajectory,
        adjoint_forcing,
    )
    from_odd = swap(block, "gy", 1, 1, False)
    from_even = swap(block, "gy", 0, 1, False)
    lon_odd = swap(strip_odd, "gx", 1, 1, True)
    lon_even = swap(strip_even, "gx", 0, 1, True)
    corner_shape = (levels + 3 * levels // 8, lat_rows, lon_cols)
    small = pltpu.CompilerParams(vmem_limit_bytes=4 * 1024 * 1024)
    corners, rims = pl.pallas_call(
        corner_odd_kernel,
        in_specs=[smem, smem] + vmem(3),
        out_specs=vmem(2),
        out_shape=[
            pltpu.VMEM(corner_shape, f32),
            pltpu.VMEM((2, lat_rows, lon_cols), f32),
        ],
        compiler_params=small,
    )(place_x, place_y, lon_odd, lon_even, from_even)
    corner_odd = swap(corners, "gy", 1, 1, False)
    corners_b = pl.pallas_call(
        corner_even_kernel,
        in_specs=[smem] + vmem(2),
        out_specs=vmem(1)[0],
        out_shape=pltpu.VMEM(corner_shape, f32),
        compiler_params=small,
    )(place_y, corners, from_odd)
    corner_even = swap(corners_b, "gy", 0, 1, False)
    scratch = [pltpu.VMEM((levels, 24, 256), f32) for _ in range(23)]
    return tuple(
        pl.pallas_call(
            solve_kernel,
            in_specs=[smem, smem, smem] + vmem(10),
            out_specs=vmem(3),
            out_shape=[jax.ShapeDtypeStruct(tile, f32)] * 3,
            scratch_shapes=scratch,
            compiler_params=pltpu.CompilerParams(vmem_limit_bytes=20 * 1024 * 1024),
        )(
            place_y,
            level_diffusion,
            damping,
            wave,
            block,
            from_odd,
            from_even,
            corners,
            corner_odd,
            corner_even,
            rims,
            observations,
            observation_weight,
        )
    )


def solution(mesh):
    spread = P(None, "gy", "gx")
    in_specs = (spread,) * 7 + (P(), P()) + (spread,) * 3 + (P(),)
    return jax.shard_map(
        compute, mesh=mesh, in_specs=in_specs, out_specs=(spread,) * 3, check_vma=False
    )
```

```python
import functools
import math

import jax
import jax.numpy as jnp
from jax import lax
from jax.experimental import pallas as pl
from jax.experimental.pallas import tpu as pltpu
from jax.sharding import PartitionSpec as P

DAY_STEPS = 96
RELAXATION = 0.7
SLOT = 8
FIELDS = 8
FORWARD = 6
C, S, ED, EW, ND, NW, TR, AF = range(8)


def lane_ids():
    return lax.broadcasted_iota(jnp.int32, (8, 128), 1)


def turned(value, shift):
    return value if shift % 128 == 0 else pltpu.roll(value, shift % 128, 1)


def pack_kernel(size_y, x_ref, y_ref, *refs):
    fields = refs[:FIELDS]
    block, block_f, strip_odd, strip_even = refs[FIELDS:]
    odd_x, last = x_ref[0] % 2 == 1, y_ref[0] == size_y - 1
    levels = fields[0].shape[0]
    half = levels // 2
    lanes = lane_ids()
    row = lax.broadcasted_iota(jnp.int32, (8, 128), 0)
    closed = jnp.where((row == 7) & last, 0.0, 1.0)
    rim_east = jnp.zeros((8, 128), jnp.float32)
    rim_west = jnp.zeros((8, 128), jnp.float32)
    for place in range(half):
        east = jnp.zeros((8, 128), jnp.float32)
        west = jnp.zeros((8, 128), jnp.float32)
        for level in (place, place + half):
            for k in range(FIELDS):
                value = fields[k][level]
                if k in (ND, NW):
                    value = value * closed
                block[k, level] = value
                if k < FORWARD:
                    block_f[k, level] = value
                base = SLOT * k + (64 if level >= half else 0)
                slot = (lanes >= base) & (lanes < base + SLOT)
                east = jnp.where(slot, turned(value, base + SLOT), east)
                west = jnp.where(slot, turned(value, base), west)
                if k == C:
                    rim_west = jnp.where(lanes == level, turned(value, level - SLOT), rim_west)
                if k in (C, ED, EW):
                    lane_at = {C: 0, ED: 1, EW: 2}[k] * levels + level
                    moved = turned(value, lane_at - (127 - SLOT))
                    rim_east = jnp.where(lanes == lane_at, moved, rim_east)
        strip_odd[place] = jnp.where(odd_x, east, west)
        strip_even[place] = jnp.where(odd_x, west, east)
    strip_odd[half] = jnp.where(odd_x, rim_east, rim_west)
    strip_even[half] = jnp.where(odd_x, rim_west, rim_east)


def relay(odd_y, high_when_odd, block, corners):
    levels = block.shape[1]
    for row in range(3 * levels):
        value = block[(C, ND, NW)[row // levels], row % levels]
        high, low = value[7:8], value[0:1]
        line = jnp.where(odd_y, high, low) if high_when_odd else jnp.where(odd_y, low, high)
        at = row % 8
        corners[levels + row // 8, at : at + 1] = line


def corner_odd_kernel(x_ref, y_ref, from_odd, from_even, block_even, block, corners, rims):
    half = from_odd.shape[0] - 1
    odd_x = x_ref[0] % 2 == 1
    for place in range(half):
        corners[place] = jnp.where(odd_x, from_even[place], from_odd[place])
        corners[half + place] = jnp.where(odd_x, from_odd[place], from_even[place])
    rims[0] = jnp.where(odd_x, from_even[half], from_odd[half])
    rims[1] = jnp.where(odd_x, from_odd[half], from_even[half])
    relay(y_ref[0] % 2 == 1, True, block_even, corners)
    levels = block.shape[1]
    base = levels + 3 * levels // 8
    for k in range(FORWARD, FIELDS):
        for level in range(levels):
            corners[base + (k - FORWARD) * levels + level] = block[k, level]


def corner_even_kernel(y_ref, corner_own, block_odd, corners):
    for place in range(block_odd.shape[1]):
        corners[place] = corner_own[place]
    relay(y_ref[0] % 2 == 1, False, block_odd, corners)


def solve_kernel(
    y_ref,
    level_ref,
    damp_ref,
    cos_ref,
    own,
    from_odd,
    from_even,
    corner_own,
    corner_odd,
    corner_even,
    rims,
    observations,
    weight,
    out_state,
    out_resid,
    out_adjoint,
    check,
    force,
    a_c,
    diag,
    up_e,
    low_w,
    up_n,
    low_s,
    low_e,
    up_w,
    low_n,
    up_s,
    wt,
    ctr,
    g,
    d,
    x,
    aq_a,
    wt_a,
    ctr_a,
    g_a,
    d_a,
    mu,
):
    levels = check.shape[0]
    lanes = lane_ids()
    rows = lax.broadcasted_iota(jnp.int32, (24, 256), 0)

    half = levels // 2
    odd_y = y_ref[0] % 2 == 1

    def odd_tile(k, at):
        if k < FORWARD:
            return from_odd[k, at]
        return corner_odd[levels + 3 * levels // 8 + (k - FORWARD) * levels + at]

    def tile_south(k, at):
        return jnp.where(odd_y, from_even[k, at], odd_tile(k, at))

    def tile_north(k, at):
        return jnp.where(odd_y, odd_tile(k, at), from_even[k, at])

    def tile_own(k, at):
        return own[k, at]

    def side_south(at):
        return jnp.where(odd_y, corner_even[at], corner_odd[at])

    def side_north(at):
        return jnp.where(odd_y, corner_odd[at], corner_even[at])

    def side_own(at):
        return corner_own[at]

    def far_south(at):
        tile, row = levels + at // 8, at % 8
        return side_south(tile)[row : row + 1]

    def far_north(at):
        tile, row = levels + at // 8, at % 8
        return side_north(tile)[row : row + 1]

    def halo(k, level, west, east):
        base = SLOT * k + (64 if level >= half else 0)
        left = turned(west, 128 - SLOT - base)
        right = turned(east, -base)
        return jnp.where(lanes < SLOT, right, jnp.where(lanes >= 128 - SLOT, left, 0.0))

    def gather(k, level):
        place = level % half
        tiles = []
        for tile, strip in (
            (tile_south, side_south),
            (tile_own, side_own),
            (tile_north, side_north),
        ):
            side = halo(k, level, strip(place), strip(half + place))
            if tile is tile_own:
                if k == C:
                    side = jnp.where(lanes == SLOT, turned(rims[1], SLOT - level), side)
                if k in (C, ED, EW):
                    lane_at = {C: 0, ED: 1, EW: 2}[k] * levels + level
                    moved = turned(rims[0], 127 - SLOT - lane_at)
                    side = jnp.where(lanes == 127 - SLOT, moved, side)
            tiles.append(jnp.concatenate([tile(k, level), side], axis=1))
        return jnp.concatenate(tiles, axis=0)

    def wide(line):
        line = jnp.concatenate([line, jnp.zeros_like(line)], axis=1)
        return jnp.broadcast_to(line, (24, 256))

    def to_e(v):
        return pltpu.roll(v, 255, 1)

    def to_w(v):
        return pltpu.roll(v, 1, 1)

    def to_n(v):
        return pltpu.roll(v, 23, 0)

    def to_s(v):
        return pltpu.roll(v, 1, 0)

    def up(level):
        return level_ref[level] if level < levels - 1 else None

    def down(level):
        return level_ref[level - 1] if level > 0 else None

    def pair(level):
        parts = [u for u in (up(level), down(level)) if u is not None]
        return sum(parts[1:], parts[0])

    def with_levels(total, level, below, above):
        if above is not None:
            total = total - up(level) * above
        if below is not None:
            total = total - down(level) * below
        return total

    def forward_sum(level, v, below, above, v_n=None, v_s=None):
        v_n = to_n(v) if v_n is None else v_n
        v_s = to_s(v) if v_s is None else v_s
        total = up_e[level] * to_e(v) - low_w[level] * to_w(v)
        total = total + (up_n[level] * v_n - low_s[level] * v_s)
        return with_levels(total, level, below, above)

    def adjoint_sum(level, v, below, above):
        total = up_w[level] * to_w(v) - low_e[level] * to_e(v)
        total = total + (up_s[level] * to_s(v) - low_n[level] * to_n(v))
        return with_levels(total, level, below, above)

    def sweep(field, body):
        below, here = None, field[0]
        for level in range(levels):
            above = field[level + 1] if level + 1 < levels else None
            body(level, here, below, above)
            below, here = here, above

    for level in range(levels):
        ed = gather(ED, level)
        ew = gather(EW, level) * 0.5
        nd = gather(ND, level)
        nw = gather(NW, level) * 0.5
        far_nd = wide(far_south(levels + level))
        far_nw = wide(far_south(2 * levels + level)) * 0.5
        first = rows == 0
        e_low, e_up, n_low, n_up = ew + ed, ew - ed, nw + nd, nw - nd
        w_low, w_up = to_w(e_low), to_w(e_up)
        s_low = jnp.where(first, far_nw + far_nd, to_s(n_low))
        s_up = jnp.where(first, far_nw - far_nd, to_s(n_up))
        up_e[level] = e_up
        low_e[level] = e_low
        up_w[level] = w_up
        low_w[level] = w_low
        up_n[level] = n_up
        low_n[level] = n_low
        up_s[level] = s_up
        low_s[level] = s_low
        center = (e_low - w_up) + (n_low - s_up) + pair(level)
        a_c[level] = center
        base = ed + to_w(ed) + nd + jnp.where(first, far_nd, to_s(nd)) + (1.0 + pair(level))
        diag[level] = base
        check[level] = gather(C, level)
        force[level] = gather(S, level) * cos_ref[...]
        tangent = jnp.tanh(gather(TR, level))
        local = damp_ref[level] * (1.0 - tangent * tangent)
        weight_a = RELAXATION / (base + local)
        af = gather(AF, level)
        diagonal = 1.0 + center + local
        aq_a[level] = diagonal
        wt_a[level] = weight_a
        ctr_a[level] = 1.0 - weight_a * diagonal
        start = weight_a * af
        g_a[level] = start
        d_a[level] = start

    def newton(level, resid, tangent):
        local = damp_ref[level] * (1.0 - tangent * tangent)
        w = RELAXATION / (diag[level] + local)
        wt[level] = w
        ctr[level] = 1.0 - w * (1.0 + a_c[level] + local)
        start = -(w * resid)
        g[level] = start
        d[level] = start

    def first_resid(level, v, below, above):
        tangent = jnp.tanh(v)
        v_s = jnp.where(rows == 0, wide(far_south(level)), to_s(v))
        v_n = jnp.where(rows == 23, wide(far_north(level)), to_n(v))
        total = forward_sum(level, v, below, above, v_n, v_s)
        resid = total + a_c[level] * v + damp_ref[level] * tangent - force[level]
        newton(level, resid, tangent)

    def forward_lin(level, v, below, above):
        total = forward_sum(level, v, below, above)
        d[level] = g[level] + ctr[level] * v - wt[level] * total

    def adjoint_lin(level, v, below, above):
        total = adjoint_sum(level, v, below, above)
        d_a[level] = g_a[level] + ctr_a[level] * v - wt_a[level] * total

    def relax(field, body):
        def step(_, carry):
            sweep(field, body)
            return carry

        lax.fori_loop(0, 3, step, 0)

    sweep(check, first_resid)
    relax(d, forward_lin)

    relax(d_a, adjoint_lin)
    for level in range(levels):
        x[level] = check[level] + d[level]
        mu[level] = d_a[level]

    def second_resid(level, v, below, above):
        tangent = jnp.tanh(v)
        total = forward_sum(level, v, below, above)
        moved = v - check[level]
        resid = moved + total + a_c[level] * v + damp_ref[level] * tangent - force[level]
        newton(level, resid, tangent)

    def adjoint_resid(level, v, below, above):
        total = adjoint_sum(level, v, below, above)
        af = g_a[level]
        start = af - wt_a[level] * (total + aq_a[level] * v)
        g_a[level] = start
        d_a[level] = start

    sweep(x, second_resid)
    relax(d, forward_lin)
    sweep(mu, adjoint_resid)
    relax(d_a, adjoint_lin)
    for level in range(levels):
        final = x[level] + d[level]
        x[level] = final
        state = final[8:16, :128]
        out_state[level] = state
        multiplier = mu[level, 8:16, :128] + d_a[level, 8:16, :128]
        out_adjoint[level] = multiplier + weight[level] * (state - observations[level])

    def final_resid(level, v, below, above):
        total = forward_sum(level, v, below, above)
        moved = v - check[level]
        resid = moved + total + a_c[level] * v + damp_ref[level] * jnp.tanh(v) - force[level]
        out_resid[level] = resid[8:16, :128]

    sweep(x, final_resid)


def vmem(count):
    return [pl.BlockSpec(memory_space=pltpu.VMEM) for _ in range(count)]


def swap(array, axis, start, step, periodic):
    size = lax.axis_size(axis)
    pairs = []
    for low in range(size):
        high = low + step
        if (low - start) % (2 * step) < step and (periodic or high < size):
            pairs += [(low, high % size), (high % size, low)]
    return lax.ppermute(array, axis, pairs)


def compute(
    checkpoint,
    trajectory,
    adjoint_forcing,
    east_diffusion,
    north_diffusion,
    east_wind,
    north_wind,
    level_diffusion,
    damping,
    source,
    observations,
    observation_weight,
    step_index,
):
    levels, lat_rows, lon_cols = checkpoint.shape
    size_x = lax.axis_size("gx")
    size_y = lax.axis_size("gy")
    lane = jnp.arange(256, dtype=jnp.int32)
    column = lax.axis_index("gx") * lon_cols + lane - jnp.where(lane >= 192, 256, 0)
    column = jnp.remainder(column, lon_cols * size_x).astype(jnp.float32)
    phase = (
        2.0 * math.pi * column / (lon_cols * size_x)
        - 2.0 * math.pi * step_index[0].astype(jnp.float32) / DAY_STEPS
    )
    wave = jnp.cos(phase)[None, :]
    index_x, index_y = lax.axis_index("gx"), lax.axis_index("gy")
    place_x = index_x.astype(jnp.int32)[None]
    place_y = index_y.astype(jnp.int32)[None]
    tile = (levels, lat_rows, lon_cols)
    f32 = jnp.float32
    smem = pl.BlockSpec(memory_space=pltpu.SMEM)
    strip = (levels // 2 + 1, lat_rows, lon_cols)
    block, block_f, strip_odd, strip_even = pl.pallas_call(
        functools.partial(pack_kernel, size_y),
        in_specs=[smem, smem] + vmem(8),
        out_specs=vmem(4),
        out_shape=[
            pltpu.VMEM((FIELDS,) + tile, f32),
            pltpu.VMEM((FORWARD,) + tile, f32),
            pltpu.VMEM(strip, f32),
            pltpu.VMEM(strip, f32),
        ],
    )(
        place_x,
        place_y,
        checkpoint,
        source,
        east_diffusion,
        east_wind,
        north_diffusion,
        north_wind,
        trajectory,
        adjoint_forcing,
    )
    from_odd = swap(block_f, "gy", 1, 1, False)
    from_even = swap(block, "gy", 0, 1, False)
    lon_odd = swap(strip_odd, "gx", 1, 1, True)
    lon_even = swap(strip_even, "gx", 0, 1, True)
    corner_shape = (levels + 3 * levels // 8, lat_rows, lon_cols)
    small = pltpu.CompilerParams(vmem_limit_bytes=4 * 1024 * 1024)
    corners, rims = pl.pallas_call(
        corner_odd_kernel,
        in_specs=[smem, smem] + vmem(4),
        out_specs=vmem(2),
        out_shape=[
            pltpu.VMEM((corner_shape[0] + 2 * levels,) + corner_shape[1:], f32),
            pltpu.VMEM((2, lat_rows, lon_cols), f32),
        ],
        compiler_params=small,
    )(place_x, place_y, lon_odd, lon_even, from_even, block)
    corner_odd = swap(corners, "gy", 1, 1, False)
    corners_b = pl.pallas_call(
        corner_even_kernel,
        in_specs=[smem] + vmem(2),
        out_specs=vmem(1)[0],
        out_shape=pltpu.VMEM(corner_shape, f32),
        compiler_params=small,
    )(place_y, corners, from_odd)
    corner_even = swap(corners_b, "gy", 0, 1, False)
    scratch = [pltpu.VMEM((levels, 24, 256), f32) for _ in range(23)]
    return tuple(
        pl.pallas_call(
            solve_kernel,
            in_specs=[smem, smem, smem] + vmem(10),
            out_specs=vmem(3),
            out_shape=[jax.ShapeDtypeStruct(tile, f32)] * 3,
            scratch_shapes=scratch,
            compiler_params=pltpu.CompilerParams(vmem_limit_bytes=20 * 1024 * 1024),
        )(
            place_y,
            level_diffusion,
            damping,
            wave,
            block,
            from_odd,
            from_even,
            corners,
            corner_odd,
            corner_even,
            rims,
            observations,
            observation_weight,
        )
    )


def solution(mesh):
    spread = P(None, "gy", "gx")
    in_specs = (spread,) * 7 + (P(), P()) + (spread,) * 3 + (P(),)
    return jax.shard_map(
        compute, mesh=mesh, in_specs=in_specs, out_specs=(spread,) * 3, check_vma=False
    )
```

```python
import functools
import math

import jax
import jax.numpy as jnp
from jax import lax
from jax.experimental import pallas as pl
from jax.experimental.pallas import tpu as pltpu
from jax.sharding import PartitionSpec as P

DAY_STEPS = 96
RELAXATION = 0.7
SLOT = 8
FIELDS = 8
FORWARD = 6
C, S, ED, EW, ND, NW, TR, AF = range(8)


def lane_ids():
    return lax.broadcasted_iota(jnp.int32, (8, 128), 1)


def turned(value, shift):
    return value if shift % 128 == 0 else pltpu.roll(value, shift % 128, 1)


def pack_kernel(size_y, x_ref, y_ref, *refs):
    fields = refs[:FIELDS]
    block, block_f, block_a, strip_odd, strip_even = refs[FIELDS:]
    odd_x, last = x_ref[0] % 2 == 1, y_ref[0] == size_y - 1
    levels = fields[0].shape[0]
    half = levels // 2
    lanes = lane_ids()
    row = lax.broadcasted_iota(jnp.int32, (8, 128), 0)
    closed = jnp.where((row == 7) & last, 0.0, 1.0)
    rim_east = jnp.zeros((8, 128), jnp.float32)
    rim_west = jnp.zeros((8, 128), jnp.float32)
    for place in range(half):
        east = jnp.zeros((8, 128), jnp.float32)
        west = jnp.zeros((8, 128), jnp.float32)
        for level in (place, place + half):
            for k in range(FIELDS):
                value = fields[k][level]
                if k in (ND, NW):
                    value = value * closed
                block[k, level] = value
                if k < FORWARD:
                    block_f[k, level] = value
                else:
                    block_a[k - FORWARD, level] = value
                base = SLOT * k + (64 if level >= half else 0)
                slot = (lanes >= base) & (lanes < base + SLOT)
                east = jnp.where(slot, turned(value, base + SLOT), east)
                west = jnp.where(slot, turned(value, base), west)
                if k == C:
                    rim_west = jnp.where(lanes == level, turned(value, level - SLOT), rim_west)
                if k in (C, ED, EW):
                    lane_at = {C: 0, ED: 1, EW: 2}[k] * levels + level
                    moved = turned(value, lane_at - (127 - SLOT))
                    rim_east = jnp.where(lanes == lane_at, moved, rim_east)
        strip_odd[place] = jnp.where(odd_x, east, west)
        strip_even[place] = jnp.where(odd_x, west, east)
    strip_odd[half] = jnp.where(odd_x, rim_east, rim_west)
    strip_even[half] = jnp.where(odd_x, rim_west, rim_east)


def relay(odd_y, high_when_odd, block, corners):
    levels = block.shape[1]
    for row in range(3 * levels):
        value = block[(C, ND, NW)[row // levels], row % levels]
        high, low = value[7:8], value[0:1]
        line = jnp.where(odd_y, high, low) if high_when_odd else jnp.where(odd_y, low, high)
        at = row % 8
        corners[levels + row // 8, at : at + 1] = line


def corner_odd_kernel(x_ref, y_ref, from_odd, from_even, block_even, corners, rims):
    half = from_odd.shape[0] - 1
    odd_x = x_ref[0] % 2 == 1
    for place in range(half):
        corners[place] = jnp.where(odd_x, from_even[place], from_odd[place])
        corners[half + place] = jnp.where(odd_x, from_odd[place], from_even[place])
    rims[0] = jnp.where(odd_x, from_even[half], from_odd[half])
    rims[1] = jnp.where(odd_x, from_odd[half], from_even[half])
    relay(y_ref[0] % 2 == 1, True, block_even, corners)


def corner_even_kernel(y_ref, corner_own, block_odd, corners):
    for place in range(block_odd.shape[1]):
        corners[place] = corner_own[place]
    relay(y_ref[0] % 2 == 1, False, block_odd, corners)


def turn_e(v):
    return pltpu.roll(v, 255, 1)


def turn_w(v):
    return pltpu.roll(v, 1, 1)


def turn_n(v):
    return pltpu.roll(v, 23, 0)


def turn_s(v):
    return pltpu.roll(v, 1, 0)


def gatherer(odd_y, own, odd_tile, from_even, corner_own, corner_odd, corner_even, rims):
    levels = own.shape[1]
    half = levels // 2
    lanes = lane_ids()

    def tile_south(k, at):
        return jnp.where(odd_y, from_even[k, at], odd_tile(k, at))

    def tile_north(k, at):
        return jnp.where(odd_y, odd_tile(k, at), from_even[k, at])

    def tile_own(k, at):
        return own[k, at]

    def side_south(at):
        return jnp.where(odd_y, corner_even[at], corner_odd[at])

    def side_north(at):
        return jnp.where(odd_y, corner_odd[at], corner_even[at])

    def side_own(at):
        return corner_own[at]

    def far_south(at):
        tile, row = levels + at // 8, at % 8
        return side_south(tile)[row : row + 1]

    def far_north(at):
        tile, row = levels + at // 8, at % 8
        return side_north(tile)[row : row + 1]

    def halo(k, level, west, east):
        base = SLOT * k + (64 if level >= half else 0)
        left = turned(west, 128 - SLOT - base)
        right = turned(east, -base)
        return jnp.where(lanes < SLOT, right, jnp.where(lanes >= 128 - SLOT, left, 0.0))

    def gather(k, level):
        place = level % half
        tiles = []
        for tile, strip in (
            (tile_south, side_south),
            (tile_own, side_own),
            (tile_north, side_north),
        ):
            side = halo(k, level, strip(place), strip(half + place))
            if tile is tile_own:
                if k == C:
                    side = jnp.where(lanes == SLOT, turned(rims[1], SLOT - level), side)
                if k in (C, ED, EW):
                    lane_at = {C: 0, ED: 1, EW: 2}[k] * levels + level
                    moved = turned(rims[0], 127 - SLOT - lane_at)
                    side = jnp.where(lanes == 127 - SLOT, moved, side)
            tiles.append(jnp.concatenate([tile(k, level), side], axis=1))
        return jnp.concatenate(tiles, axis=0)

    return gather, far_south, far_north


def level_pair(level_ref, level, levels):
    parts = []
    if level < levels - 1:
        parts.append(level_ref[level])
    if level > 0:
        parts.append(level_ref[level - 1])
    return sum(parts[1:], parts[0])


def with_levels(level_ref, total, level, below, above):
    if above is not None:
        total = total - level_ref[level] * above
    if below is not None:
        total = total - level_ref[level - 1] * below
    return total


def sweep(field, body):
    levels = field.shape[0]
    below, here = None, field[0]
    for level in range(levels):
        above = field[level + 1] if level + 1 < levels else None
        body(level, here, below, above)
        below, here = here, above


def relax(field, body):
    def step(_, carry):
        sweep(field, body)
        return carry

    lax.fori_loop(0, 3, step, 0)


def forward_kernel(
    y_ref,
    level_ref,
    damp_ref,
    cos_ref,
    own,
    from_odd,
    from_even,
    corner_own,
    corner_odd,
    corner_even,
    rims,
    out_state,
    out_resid,
    keep_state,
    a_c,
    diag,
    low_e,
    up_w,
    low_n,
    up_s,
    check,
    force,
    up_e,
    low_w,
    up_n,
    low_s,
    wt,
    ctr,
    g,
    d,
    x,
):
    levels = check.shape[0]
    rows = lax.broadcasted_iota(jnp.int32, (24, 256), 0)
    gather, far_south, far_north = gatherer(
        y_ref[0] % 2 == 1,
        own,
        lambda k, at: from_odd[k, at],
        from_even,
        corner_own,
        corner_odd,
        corner_even,
        rims,
    )

    def wide(line):
        line = jnp.concatenate([line, jnp.zeros_like(line)], axis=1)
        return jnp.broadcast_to(line, (24, 256))

    def forward_sum(level, v, below, above, v_n=None, v_s=None):
        v_n = turn_n(v) if v_n is None else v_n
        v_s = turn_s(v) if v_s is None else v_s
        total = up_e[level] * turn_e(v) - low_w[level] * turn_w(v)
        total = total + (up_n[level] * v_n - low_s[level] * v_s)
        return with_levels(level_ref, total, level, below, above)

    for level in range(levels):
        ed = gather(ED, level)
        ew = gather(EW, level) * 0.5
        nd = gather(ND, level)
        nw = gather(NW, level) * 0.5
        far_nd = wide(far_south(levels + level))
        far_nw = wide(far_south(2 * levels + level)) * 0.5
        first = rows == 0
        e_low, e_up, n_low, n_up = ew + ed, ew - ed, nw + nd, nw - nd
        w_low, w_up = turn_w(e_low), turn_w(e_up)
        s_low = jnp.where(first, far_nw + far_nd, turn_s(n_low))
        s_up = jnp.where(first, far_nw - far_nd, turn_s(n_up))
        up_e[level] = e_up
        low_e[level] = e_low
        up_w[level] = w_up
        low_w[level] = w_low
        up_n[level] = n_up
        low_n[level] = n_low
        up_s[level] = s_up
        low_s[level] = s_low
        pair = level_pair(level_ref, level, levels)
        a_c[level] = (e_low - w_up) + (n_low - s_up) + pair
        diag[level] = ed + turn_w(ed) + nd + jnp.where(first, far_nd, turn_s(nd)) + (1.0 + pair)
        check[level] = gather(C, level)
        force[level] = gather(S, level) * cos_ref[...]

    def newton(level, resid, tangent):
        local = damp_ref[level] * (1.0 - tangent * tangent)
        w = RELAXATION / (diag[level] + local)
        wt[level] = w
        ctr[level] = 1.0 - w * (1.0 + a_c[level] + local)
        start = -(w * resid)
        g[level] = start
        d[level] = start

    def first_resid(level, v, below, above):
        tangent = jnp.tanh(v)
        v_s = jnp.where(rows == 0, wide(far_south(level)), turn_s(v))
        v_n = jnp.where(rows == 23, wide(far_north(level)), turn_n(v))
        total = forward_sum(level, v, below, above, v_n, v_s)
        resid = total + a_c[level] * v + damp_ref[level] * tangent - force[level]
        newton(level, resid, tangent)

    def forward_lin(level, v, below, above):
        total = forward_sum(level, v, below, above)
        d[level] = g[level] + ctr[level] * v - wt[level] * total

    def second_resid(level, v, below, above):
        tangent = jnp.tanh(v)
        total = forward_sum(level, v, below, above)
        moved = v - check[level]
        resid = moved + total + a_c[level] * v + damp_ref[level] * tangent - force[level]
        newton(level, resid, tangent)

    def final_resid(level, v, below, above):
        total = forward_sum(level, v, below, above)
        moved = v - check[level]
        resid = moved + total + a_c[level] * v + damp_ref[level] * jnp.tanh(v) - force[level]
        out_resid[level] = resid[8:16, :128]

    sweep(check, first_resid)
    relax(d, forward_lin)
    for level in range(levels):
        x[level] = check[level] + d[level]
    sweep(x, second_resid)
    relax(d, forward_lin)
    for level in range(levels):
        final = x[level] + d[level]
        x[level] = final
        out_state[level] = final[8:16, :128]
        keep_state[level] = final[8:16, :128]
    sweep(x, final_resid)


def adjoint_kernel(
    y_ref,
    level_ref,
    damp_ref,
    own,
    adjoint_odd,
    from_even,
    corner_own,
    corner_odd,
    corner_even,
    state,
    a_c,
    diag,
    low_e,
    up_w,
    low_n,
    up_s,
    observations,
    weight,
    out_adjoint,
    aq,
    wt,
    ctr,
    g,
    d,
    mu,
):
    levels = mu.shape[0]
    gather, _, _ = gatherer(
        y_ref[0] % 2 == 1,
        own,
        lambda k, at: adjoint_odd[k - FORWARD, at],
        from_even,
        corner_own,
        corner_odd,
        corner_even,
        None,
    )

    def adjoint_sum(level, v, below, above):
        total = up_w[level] * turn_w(v) - low_e[level] * turn_e(v)
        total = total + (up_s[level] * turn_s(v) - low_n[level] * turn_n(v))
        return with_levels(level_ref, total, level, below, above)

    for level in range(levels):
        tangent = jnp.tanh(gather(TR, level))
        local = damp_ref[level] * (1.0 - tangent * tangent)
        w = RELAXATION / (diag[level] + local)
        diagonal = 1.0 + a_c[level] + local
        aq[level] = diagonal
        wt[level] = w
        ctr[level] = 1.0 - w * diagonal
        start = w * gather(AF, level)
        g[level] = start
        d[level] = start

    def adjoint_lin(level, v, below, above):
        total = adjoint_sum(level, v, below, above)
        d[level] = g[level] + ctr[level] * v - wt[level] * total

    def adjoint_resid(level, v, below, above):
        total = adjoint_sum(level, v, below, above)
        start = g[level] - wt[level] * (total + aq[level] * v)
        g[level] = start
        d[level] = start

    relax(d, adjoint_lin)
    for level in range(levels):
        mu[level] = d[level]
    sweep(mu, adjoint_resid)
    relax(d, adjoint_lin)
    for level in range(levels):
        multiplier = mu[level, 8:16, :128] + d[level, 8:16, :128]
        out_adjoint[level] = multiplier + weight[level] * (state[level] - observations[level])


def vmem(count):
    return [pl.BlockSpec(memory_space=pltpu.VMEM) for _ in range(count)]


def swap(array, axis, start, step, periodic):
    size = lax.axis_size(axis)
    pairs = []
    for low in range(size):
        high = low + step
        if (low - start) % (2 * step) < step and (periodic or high < size):
            pairs += [(low, high % size), (high % size, low)]
    return lax.ppermute(array, axis, pairs)


def compute(
    checkpoint,
    trajectory,
    adjoint_forcing,
    east_diffusion,
    north_diffusion,
    east_wind,
    north_wind,
    level_diffusion,
    damping,
    source,
    observations,
    observation_weight,
    step_index,
):
    levels, lat_rows, lon_cols = checkpoint.shape
    size_x = lax.axis_size("gx")
    size_y = lax.axis_size("gy")
    lane = jnp.arange(256, dtype=jnp.int32)
    column = lax.axis_index("gx") * lon_cols + lane - jnp.where(lane >= 192, 256, 0)
    column = jnp.remainder(column, lon_cols * size_x).astype(jnp.float32)
    phase = (
        2.0 * math.pi * column / (lon_cols * size_x)
        - 2.0 * math.pi * step_index[0].astype(jnp.float32) / DAY_STEPS
    )
    wave = jnp.cos(phase)[None, :]
    index_x, index_y = lax.axis_index("gx"), lax.axis_index("gy")
    place_x = index_x.astype(jnp.int32)[None]
    place_y = index_y.astype(jnp.int32)[None]
    tile = (levels, lat_rows, lon_cols)
    f32 = jnp.float32
    smem = pl.BlockSpec(memory_space=pltpu.SMEM)
    strip = (levels // 2 + 1, lat_rows, lon_cols)
    block, block_f, block_a, strip_odd, strip_even = pl.pallas_call(
        functools.partial(pack_kernel, size_y),
        in_specs=[smem, smem] + vmem(8),
        out_specs=vmem(5),
        out_shape=[
            pltpu.VMEM((FIELDS,) + tile, f32),
            pltpu.VMEM((FORWARD,) + tile, f32),
            pltpu.VMEM((FIELDS - FORWARD,) + tile, f32),
            pltpu.VMEM(strip, f32),
            pltpu.VMEM(strip, f32),
        ],
    )(
        place_x,
        place_y,
        checkpoint,
        source,
        east_diffusion,
        east_wind,
        north_diffusion,
        north_wind,
        trajectory,
        adjoint_forcing,
    )
    from_odd = swap(block_f, "gy", 1, 1, False)
    from_even = swap(block, "gy", 0, 1, False)
    lon_odd = swap(strip_odd, "gx", 1, 1, True)
    lon_even = swap(strip_even, "gx", 0, 1, True)
    corner_shape = (levels + 3 * levels // 8, lat_rows, lon_cols)
    small = pltpu.CompilerParams(vmem_limit_bytes=4 * 1024 * 1024)
    corners, rims = pl.pallas_call(
        corner_odd_kernel,
        in_specs=[smem, smem] + vmem(3),
        out_specs=vmem(2),
        out_shape=[
            pltpu.VMEM(corner_shape, f32),
            pltpu.VMEM((2, lat_rows, lon_cols), f32),
        ],
        compiler_params=small,
    )(place_x, place_y, lon_odd, lon_even, from_even)
    corner_odd = swap(corners, "gy", 1, 1, False)
    corners_b = pl.pallas_call(
        corner_even_kernel,
        in_specs=[smem] + vmem(2),
        out_specs=vmem(1)[0],
        out_shape=pltpu.VMEM(corner_shape, f32),
        compiler_params=small,
    )(place_y, corners, from_odd)
    corner_even = swap(corners_b, "gy", 0, 1, False)
    adjoint_odd = swap(block_a, "gy", 1, 1, False)
    wide = (levels, 3 * lat_rows, 2 * lon_cols)
    large = pltpu.CompilerParams(vmem_limit_bytes=16 * 1024 * 1024)
    state, resid, keep_state, *coefs = pl.pallas_call(
        forward_kernel,
        in_specs=[smem] * 3 + vmem(8),
        out_specs=vmem(9),
        out_shape=[jax.ShapeDtypeStruct(tile, f32)] * 2
        + [pltpu.VMEM(tile, f32)]
        + [pltpu.VMEM(wide, f32)] * 6,
        scratch_shapes=[pltpu.VMEM(wide, f32) for _ in range(11)],
        compiler_params=large,
    )(
        place_y,
        level_diffusion,
        damping,
        wave,
        block,
        from_odd,
        from_even,
        corners,
        corner_odd,
        corner_even,
        rims,
    )
    result = pl.pallas_call(
        adjoint_kernel,
        in_specs=[smem] * 3 + vmem(15),
        out_specs=vmem(1)[0],
        out_shape=jax.ShapeDtypeStruct(tile, f32),
        scratch_shapes=[pltpu.VMEM(wide, f32) for _ in range(6)],
        compiler_params=large,
    )(
        place_y,
        level_diffusion,
        damping,
        block,
        adjoint_odd,
        from_even,
        corners,
        corner_odd,
        corner_even,
        keep_state,
        *coefs,
        observations,
        observation_weight,
    )
    return state, resid, result


def solution(mesh):
    spread = P(None, "gy", "gx")
    in_specs = (spread,) * 7 + (P(), P()) + (spread,) * 3 + (P(),)
    return jax.shard_map(
        compute, mesh=mesh, in_specs=in_specs, out_specs=(spread,) * 3, check_vma=False
    )
```

```python
import functools
import math

import jax
import jax.numpy as jnp
from jax import lax
from jax.experimental import pallas as pl
from jax.experimental.pallas import tpu as pltpu
from jax.sharding import PartitionSpec as P

DAY_STEPS = 96
RELAXATION = 0.7
SLOT = 8
FIELDS = 8
FORWARD = 6
C, S, ED, EW, ND, NW, TR, AF = range(8)


def lane_ids():
    return lax.broadcasted_iota(jnp.int32, (8, 128), 1)


def turned(value, shift):
    return value if shift % 128 == 0 else pltpu.roll(value, shift % 128, 1)


def pack_kernel(size_y, x_ref, y_ref, *refs):
    fields = refs[:FIELDS]
    block, block_f, strip_odd, strip_even = refs[FIELDS:]
    odd_x, last = x_ref[0] % 2 == 1, y_ref[0] == size_y - 1
    levels = fields[0].shape[0]
    half = levels // 2
    lanes = lane_ids()
    row = lax.broadcasted_iota(jnp.int32, (8, 128), 0)
    closed = jnp.where((row == 7) & last, 0.0, 1.0)
    rim_east = jnp.zeros((8, 128), jnp.float32)
    rim_west = jnp.zeros((8, 128), jnp.float32)
    for place in range(half):
        east = jnp.zeros((8, 128), jnp.float32)
        west = jnp.zeros((8, 128), jnp.float32)
        for level in (place, place + half):
            for k in range(FIELDS):
                value = fields[k][level]
                if k in (ND, NW):
                    value = value * closed
                block[k, level] = value
                if k < FORWARD:
                    block_f[k, level] = value
                base = SLOT * k + (64 if level >= half else 0)
                slot = (lanes >= base) & (lanes < base + SLOT)
                east = jnp.where(slot, turned(value, base + SLOT), east)
                west = jnp.where(slot, turned(value, base), west)
                if k == C:
                    rim_west = jnp.where(lanes == level, turned(value, level - SLOT), rim_west)
                if k in (C, ED, EW):
                    lane_at = {C: 0, ED: 1, EW: 2}[k] * levels + level
                    moved = turned(value, lane_at - (127 - SLOT))
                    rim_east = jnp.where(lanes == lane_at, moved, rim_east)
        strip_odd[place] = jnp.where(odd_x, east, west)
        strip_even[place] = jnp.where(odd_x, west, east)
    strip_odd[half] = jnp.where(odd_x, rim_east, rim_west)
    strip_even[half] = jnp.where(odd_x, rim_west, rim_east)


def relay(odd_y, high_when_odd, block, corners):
    levels = block.shape[1]
    for row in range(3 * levels):
        value = block[(C, ND, NW)[row // levels], row % levels]
        high, low = value[7:8], value[0:1]
        line = jnp.where(odd_y, high, low) if high_when_odd else jnp.where(odd_y, low, high)
        at = row % 8
        corners[levels + row // 8, at : at + 1] = line


def corner_odd_kernel(x_ref, y_ref, from_odd, from_even, block_even, block, corners, rims):
    half = from_odd.shape[0] - 1
    odd_x = x_ref[0] % 2 == 1
    for place in range(half):
        corners[place] = jnp.where(odd_x, from_even[place], from_odd[place])
        corners[half + place] = jnp.where(odd_x, from_odd[place], from_even[place])
    rims[0] = jnp.where(odd_x, from_even[half], from_odd[half])
    rims[1] = jnp.where(odd_x, from_odd[half], from_even[half])
    relay(y_ref[0] % 2 == 1, True, block_even, corners)
    levels = block.shape[1]
    base = levels + 3 * levels // 8
    for k in range(FORWARD, FIELDS):
        for level in range(levels):
            corners[base + (k - FORWARD) * levels + level] = block[k, level]


def corner_even_kernel(y_ref, corner_own, block_odd, corners):
    for place in range(block_odd.shape[1]):
        corners[place] = corner_own[place]
    relay(y_ref[0] % 2 == 1, False, block_odd, corners)


def solve_kernel(
    y_ref,
    level_ref,
    damp_ref,
    cos_ref,
    own,
    from_odd,
    from_even,
    corner_own,
    corner_odd,
    corner_even,
    rims,
    observations,
    weight,
    out_state,
    out_resid,
    out_adjoint,
    check,
    d,
    x,
    d_a,
    mu,
    up_n,
    low_n,
    north,
    force,
    a_c,
    diag,
    up_e,
    low_w,
    low_e,
    up_w,
    wt,
    ctr,
    g,
    aq_a,
    wt_a,
    ctr_a,
    g_a,
):
    levels = check.shape[0]
    lanes = lane_ids()

    half = levels // 2
    odd_y = y_ref[0] % 2 == 1

    def odd_tile(k, at):
        if k < FORWARD:
            return from_odd[k, at]
        return corner_odd[levels + 3 * levels // 8 + (k - FORWARD) * levels + at]

    def tile_south(k, at):
        return jnp.where(odd_y, from_even[k, at], odd_tile(k, at))

    def tile_north(k, at):
        return jnp.where(odd_y, odd_tile(k, at), from_even[k, at])

    def tile_own(k, at):
        return own[k, at]

    def side_south(at):
        return jnp.where(odd_y, corner_even[at], corner_odd[at])

    def side_north(at):
        return jnp.where(odd_y, corner_odd[at], corner_even[at])

    def side_own(at):
        return corner_own[at]

    def far_south(at):
        tile, row = levels + at // 8, at % 8
        return side_south(tile)[row : row + 1]

    def far_north(at):
        tile, row = levels + at // 8, at % 8
        return side_north(tile)[row : row + 1]

    def halo(k, level, west, east):
        base = SLOT * k + (64 if level >= half else 0)
        left = turned(west, 128 - SLOT - base)
        right = turned(east, -base)
        return jnp.where(lanes < SLOT, right, jnp.where(lanes >= 128 - SLOT, left, 0.0))

    def strips(level):
        place = level % half
        pairs = []
        for side in (side_south, side_own, side_north):
            pairs.append((side(place), side(half + place)))
        return pairs

    def gather(k, level, pairs):
        tiles = []
        for tile, (west, east) in zip((tile_south, tile_own, tile_north), pairs):
            side = halo(k, level, west, east)
            if tile is tile_own:
                if k == C:
                    side = jnp.where(lanes == SLOT, turned(rims[1], SLOT - level), side)
                if k in (C, ED, EW):
                    lane_at = {C: 0, ED: 1, EW: 2}[k] * levels + level
                    moved = turned(rims[0], 127 - SLOT - lane_at)
                    side = jnp.where(lanes == 127 - SLOT, moved, side)
            tiles.append(jnp.concatenate([tile(k, level), side], axis=1))
        return jnp.concatenate(tiles, axis=0)

    def rows_of(ref, level, first):
        parts = [ref[level, side, first : first + 24] for side in range(2)]
        return jnp.concatenate(parts, axis=1)

    def middle(ref, level):
        return rows_of(ref, level, 8)

    def to_n(ref, level):
        return rows_of(ref, level, 9)

    def to_s(ref, level):
        return rows_of(ref, level, 7)

    def keep(ref, level, value):
        ref[level, 0, 8:32] = value[:, :128]
        ref[level, 1, 8:32] = value[:, 128:]

    def to_e(v):
        return pltpu.roll(v, 255, 1)

    def to_w(v):
        return pltpu.roll(v, 1, 1)

    def up(level):
        return level_ref[level] if level < levels - 1 else None

    def down(level):
        return level_ref[level - 1] if level > 0 else None

    def pair(level):
        parts = [u for u in (up(level), down(level)) if u is not None]
        return sum(parts[1:], parts[0])

    def with_levels(total, level, below, above):
        if above is not None:
            total = total - up(level) * above
        if below is not None:
            total = total - down(level) * below
        return total

    def forward_sum(field, level, v, below, above):
        total = up_e[level] * to_e(v) - low_w[level] * to_w(v)
        rows_n = middle(up_n, level) * to_n(field, level)
        total = total + (rows_n - to_s(low_n, level) * to_s(field, level))
        return with_levels(total, level, below, above)

    def adjoint_sum(field, level, v, below, above):
        total = up_w[level] * to_w(v) - low_e[level] * to_e(v)
        rows_s = to_s(up_n, level) * to_s(field, level)
        total = total + (rows_s - middle(low_n, level) * to_n(field, level))
        return with_levels(total, level, below, above)

    def sweep(field, body):
        below, here = None, middle(field, 0)
        for level in range(levels):
            above = middle(field, level + 1) if level + 1 < levels else None
            body(field, level, here, below, above)
            below, here = here, above

    blank = jnp.zeros((8, 128), jnp.float32)
    for ref in (check, d, x, d_a, mu, up_n, low_n, north):
        for level in range(levels):
            for side in range(2):
                ref[level, side, 0:8] = blank
                ref[level, side, 32:40] = blank

    for level in range(levels):
        pairs = strips(level)
        ed = gather(ED, level, pairs)
        ew = gather(EW, level, pairs) * 0.5
        nd = gather(ND, level, pairs)
        nw = gather(NW, level, pairs) * 0.5
        far_nd = far_south(levels + level)
        far_nw = far_south(2 * levels + level) * 0.5
        e_low, e_up, n_low, n_up = ew + ed, ew - ed, nw + nd, nw - nd
        keep(up_n, level, n_up)
        keep(low_n, level, n_low)
        keep(north, level, nd)
        up_n[level, 0, 7:8] = far_nw - far_nd
        low_n[level, 0, 7:8] = far_nw + far_nd
        north[level, 0, 7:8] = far_nd
        w_low, w_up = to_w(e_low), to_w(e_up)
        up_e[level] = e_up
        low_e[level] = e_low
        up_w[level] = w_up
        low_w[level] = w_low
        center = (e_low - w_up) + (n_low - to_s(up_n, level)) + pair(level)
        a_c[level] = center
        base = ed + to_w(ed) + nd + to_s(north, level) + (1.0 + pair(level))
        diag[level] = base
        keep(check, level, gather(C, level, pairs))
        check[level, 0, 7:8] = far_south(level)
        check[level, 0, 32:33] = far_north(level)
        force[level] = gather(S, level, pairs) * cos_ref[...]
        tangent = jnp.tanh(gather(TR, level, pairs))
        local = damp_ref[level] * (1.0 - tangent * tangent)
        weight_a = RELAXATION / (base + local)
        af = gather(AF, level, pairs)
        diagonal = 1.0 + center + local
        aq_a[level] = diagonal
        wt_a[level] = weight_a
        ctr_a[level] = 1.0 - weight_a * diagonal
        start = weight_a * af
        g_a[level] = start
        keep(d_a, level, start)

    def newton(level, resid, tangent):
        local = damp_ref[level] * (1.0 - tangent * tangent)
        w = RELAXATION / (diag[level] + local)
        wt[level] = w
        ctr[level] = 1.0 - w * (1.0 + a_c[level] + local)
        start = -(w * resid)
        g[level] = start
        keep(d, level, start)

    def first_resid(field, level, v, below, above):
        tangent = jnp.tanh(v)
        total = forward_sum(field, level, v, below, above)
        resid = total + a_c[level] * v + damp_ref[level] * tangent - force[level]
        newton(level, resid, tangent)

    def forward_lin(field, level, v, below, above):
        total = forward_sum(field, level, v, below, above)
        keep(field, level, g[level] + ctr[level] * v - wt[level] * total)

    def adjoint_lin(field, level, v, below, above):
        total = adjoint_sum(field, level, v, below, above)
        keep(field, level, g_a[level] + ctr_a[level] * v - wt_a[level] * total)

    def relax(field, body):
        def step(_, carry):
            sweep(field, body)
            return carry

        lax.fori_loop(0, 3, step, 0)

    sweep(check, first_resid)
    relax(d, forward_lin)
    relax(d_a, adjoint_lin)
    for level in range(levels):
        keep(x, level, middle(check, level) + middle(d, level))
        keep(mu, level, middle(d_a, level))

    def second_resid(field, level, v, below, above):
        tangent = jnp.tanh(v)
        total = forward_sum(field, level, v, below, above)
        moved = v - middle(check, level)
        resid = moved + total + a_c[level] * v + damp_ref[level] * tangent - force[level]
        newton(level, resid, tangent)

    def adjoint_resid(field, level, v, below, above):
        total = adjoint_sum(field, level, v, below, above)
        start = g_a[level] - wt_a[level] * (total + aq_a[level] * v)
        g_a[level] = start
        keep(d_a, level, start)

    sweep(x, second_resid)
    relax(d, forward_lin)
    sweep(mu, adjoint_resid)
    relax(d_a, adjoint_lin)
    for level in range(levels):
        final = middle(x, level) + middle(d, level)
        keep(x, level, final)
        state = final[8:16, :128]
        out_state[level] = state
        multiplier = mu[level, 0, 16:24] + d_a[level, 0, 16:24]
        out_adjoint[level] = multiplier + weight[level] * (state - observations[level])

    def final_resid(field, level, v, below, above):
        total = forward_sum(field, level, v, below, above)
        moved = v - middle(check, level)
        resid = moved + total + a_c[level] * v + damp_ref[level] * jnp.tanh(v) - force[level]
        out_resid[level] = resid[8:16, :128]

    sweep(x, final_resid)


def vmem(count):
    return [pl.BlockSpec(memory_space=pltpu.VMEM) for _ in range(count)]


def swap(array, axis, start, step, periodic):
    size = lax.axis_size(axis)
    pairs = []
    for low in range(size):
        high = low + step
        if (low - start) % (2 * step) < step and (periodic or high < size):
            pairs += [(low, high % size), (high % size, low)]
    return lax.ppermute(array, axis, pairs)


def compute(
    checkpoint,
    trajectory,
    adjoint_forcing,
    east_diffusion,
    north_diffusion,
    east_wind,
    north_wind,
    level_diffusion,
    damping,
    source,
    observations,
    observation_weight,
    step_index,
):
    levels, lat_rows, lon_cols = checkpoint.shape
    size_x = lax.axis_size("gx")
    size_y = lax.axis_size("gy")
    lane = jnp.arange(256, dtype=jnp.int32)
    column = lax.axis_index("gx") * lon_cols + lane - jnp.where(lane >= 192, 256, 0)
    column = jnp.remainder(column, lon_cols * size_x).astype(jnp.float32)
    phase = (
        2.0 * math.pi * column / (lon_cols * size_x)
        - 2.0 * math.pi * step_index[0].astype(jnp.float32) / DAY_STEPS
    )
    wave = jnp.cos(phase)[None, :]
    index_x, index_y = lax.axis_index("gx"), lax.axis_index("gy")
    place_x = index_x.astype(jnp.int32)[None]
    place_y = index_y.astype(jnp.int32)[None]
    tile = (levels, lat_rows, lon_cols)
    f32 = jnp.float32
    smem = pl.BlockSpec(memory_space=pltpu.SMEM)
    strip = (levels // 2 + 1, lat_rows, lon_cols)
    block, block_f, strip_odd, strip_even = pl.pallas_call(
        functools.partial(pack_kernel, size_y),
        in_specs=[smem, smem] + vmem(8),
        out_specs=vmem(4),
        out_shape=[
            pltpu.VMEM((FIELDS,) + tile, f32),
            pltpu.VMEM((FORWARD,) + tile, f32),
            pltpu.VMEM(strip, f32),
            pltpu.VMEM(strip, f32),
        ],
    )(
        place_x,
        place_y,
        checkpoint,
        source,
        east_diffusion,
        east_wind,
        north_diffusion,
        north_wind,
        trajectory,
        adjoint_forcing,
    )
    from_odd = swap(block_f, "gy", 1, 1, False)
    from_even = swap(block, "gy", 0, 1, False)
    lon_odd = swap(strip_odd, "gx", 1, 1, True)
    lon_even = swap(strip_even, "gx", 0, 1, True)
    corner_shape = (levels + 3 * levels // 8, lat_rows, lon_cols)
    small = pltpu.CompilerParams(vmem_limit_bytes=4 * 1024 * 1024)
    corners, rims = pl.pallas_call(
        corner_odd_kernel,
        in_specs=[smem, smem] + vmem(4),
        out_specs=vmem(2),
        out_shape=[
            pltpu.VMEM((corner_shape[0] + 2 * levels,) + corner_shape[1:], f32),
            pltpu.VMEM((2, lat_rows, lon_cols), f32),
        ],
        compiler_params=small,
    )(place_x, place_y, lon_odd, lon_even, from_even, block)
    corner_odd = swap(corners, "gy", 1, 1, False)
    corners_b = pl.pallas_call(
        corner_even_kernel,
        in_specs=[smem] + vmem(2),
        out_specs=vmem(1)[0],
        out_shape=pltpu.VMEM(corner_shape, f32),
        compiler_params=small,
    )(place_y, corners, from_odd)
    corner_even = swap(corners_b, "gy", 0, 1, False)
    scratch = [pltpu.VMEM((levels, 2, 40, 128), f32) for _ in range(8)]
    scratch += [pltpu.VMEM((levels, 24, 256), f32) for _ in range(14)]
    return tuple(
        pl.pallas_call(
            solve_kernel,
            in_specs=[smem, smem, smem] + vmem(10),
            out_specs=vmem(3),
            out_shape=[jax.ShapeDtypeStruct(tile, f32)] * 3,
            scratch_shapes=scratch,
            compiler_params=pltpu.CompilerParams(vmem_limit_bytes=20 * 1024 * 1024),
        )(
            place_y,
            level_diffusion,
            damping,
            wave,
            block,
            from_odd,
            from_even,
            corners,
            corner_odd,
            corner_even,
            rims,
            observations,
            observation_weight,
        )
    )


def solution(mesh):
    spread = P(None, "gy", "gx")
    in_specs = (spread,) * 7 + (P(), P()) + (spread,) * 3 + (P(),)
    return jax.shard_map(
        compute, mesh=mesh, in_specs=in_specs, out_specs=(spread,) * 3, check_vma=False
    )
```

```python
import functools
import math

import jax
import jax.numpy as jnp
from jax import lax
from jax.experimental import pallas as pl
from jax.experimental.pallas import tpu as pltpu
from jax.sharding import PartitionSpec as P

DAY_STEPS = 96
RELAXATION = 0.7
SLOT = 8
FIELDS = 8
FORWARD = 6
C, S, ED, EW, ND, NW, TR, AF = range(8)


def lane_ids():
    return lax.broadcasted_iota(jnp.int32, (8, 128), 1)


def turned(value, shift):
    return value if shift % 128 == 0 else pltpu.roll(value, shift % 128, 1)


def pack_kernel(size_y, x_ref, y_ref, *refs):
    fields = refs[:FIELDS]
    block, block_f, strip_odd, strip_even = refs[FIELDS:]
    odd_x, last = x_ref[0] % 2 == 1, y_ref[0] == size_y - 1
    levels = fields[0].shape[0]
    half = levels // 2
    lanes = lane_ids()
    row = lax.broadcasted_iota(jnp.int32, (8, 128), 0)
    closed = jnp.where((row == 7) & last, 0.0, 1.0)
    rim_east = jnp.zeros((8, 128), jnp.float32)
    rim_west = jnp.zeros((8, 128), jnp.float32)
    for place in range(half):
        east = jnp.zeros((8, 128), jnp.float32)
        west = jnp.zeros((8, 128), jnp.float32)
        for level in (place, place + half):
            for k in range(FIELDS):
                value = fields[k][level]
                if k in (ND, NW):
                    value = value * closed
                block[k, level] = value
                if k < FORWARD:
                    block_f[k, level] = value
                base = SLOT * k + (64 if level >= half else 0)
                slot = (lanes >= base) & (lanes < base + SLOT)
                east = jnp.where(slot, turned(value, base + SLOT), east)
                west = jnp.where(slot, turned(value, base), west)
                if k == C:
                    rim_west = jnp.where(lanes == level, turned(value, level - SLOT), rim_west)
                if k in (C, ED, EW):
                    lane_at = {C: 0, ED: 1, EW: 2}[k] * levels + level
                    moved = turned(value, lane_at - (127 - SLOT))
                    rim_east = jnp.where(lanes == lane_at, moved, rim_east)
        strip_odd[place] = jnp.where(odd_x, east, west)
        strip_even[place] = jnp.where(odd_x, west, east)
    strip_odd[half] = jnp.where(odd_x, rim_east, rim_west)
    strip_even[half] = jnp.where(odd_x, rim_west, rim_east)


def relay(odd_y, high_when_odd, block, corners):
    levels = block.shape[1]
    for row in range(3 * levels):
        value = block[(C, ND, NW)[row // levels], row % levels]
        high, low = value[7:8], value[0:1]
        line = jnp.where(odd_y, high, low) if high_when_odd else jnp.where(odd_y, low, high)
        at = row % 8
        corners[levels + row // 8, at : at + 1] = line


def corner_odd_kernel(x_ref, y_ref, from_odd, from_even, block_even, block, corners, rims, parity):
    half = from_odd.shape[0] - 1
    odd_x = x_ref[0] % 2 == 1
    for place in range(half):
        corners[place] = jnp.where(odd_x, from_even[place], from_odd[place])
        corners[half + place] = jnp.where(odd_x, from_odd[place], from_even[place])
    parity[...] = jnp.where(y_ref[0] % 2 == 1, 1.0, jnp.zeros((8, 128), jnp.float32))
    rims[0] = jnp.where(odd_x, from_even[half], from_odd[half])
    rims[1] = jnp.where(odd_x, from_odd[half], from_even[half])
    relay(y_ref[0] % 2 == 1, True, block_even, corners)
    levels = block.shape[1]
    base = levels + 3 * levels // 8
    for k in range(FORWARD, FIELDS):
        for level in range(levels):
            corners[base + (k - FORWARD) * levels + level] = block[k, level]


def corner_even_kernel(y_ref, level_ref, damp_ref, corner_own, block_odd, corners, table):
    for level in range(block_odd.shape[1]):
        table[0, level] = level_ref[level]
        table[1, level] = damp_ref[level]
    for place in range(block_odd.shape[1]):
        corners[place] = corner_own[place]
    relay(y_ref[0] % 2 == 1, False, block_odd, corners)


def solve_kernel(
    table,
    cos_ref,
    parity,
    own,
    from_odd,
    from_even,
    corner_own,
    corner_odd,
    corner_even,
    rims,
    observations,
    weight,
    out_state,
    out_resid,
    out_adjoint,
    check,
    d,
    x,
    d_a,
    mu,
    up_n,
    low_n,
    north,
    force,
    a_c,
    diag,
    up_e,
    low_w,
    low_e,
    up_w,
    wt,
    ctr,
    g,
    aq_a,
    wt_a,
    ctr_a,
    g_a,
):
    levels = check.shape[0]
    lanes = lane_ids()

    half = levels // 2
    odd_y = parity[...] > 0.5

    def odd_tile(k, at):
        if k < FORWARD:
            return from_odd[k, at]
        return corner_odd[levels + 3 * levels // 8 + (k - FORWARD) * levels + at]

    def tile_south(k, at):
        return jnp.where(odd_y, from_even[k, at], odd_tile(k, at))

    def tile_north(k, at):
        return jnp.where(odd_y, odd_tile(k, at), from_even[k, at])

    def tile_own(k, at):
        return own[k, at]

    def side_south(at):
        return jnp.where(odd_y, corner_even[at], corner_odd[at])

    def side_north(at):
        return jnp.where(odd_y, corner_odd[at], corner_even[at])

    def side_own(at):
        return corner_own[at]

    def far_south(at):
        tile, row = levels + at // 8, at % 8
        return side_south(tile)[row : row + 1]

    def far_north(at):
        tile, row = levels + at // 8, at % 8
        return side_north(tile)[row : row + 1]

    def halo(k, level, west, east):
        base = SLOT * k + (64 if level >= half else 0)
        left = turned(west, 128 - SLOT - base)
        right = turned(east, -base)
        return jnp.where(lanes < SLOT, right, jnp.where(lanes >= 128 - SLOT, left, 0.0))

    def strips(level):
        place = level % half
        pairs = []
        for side in (side_south, side_own, side_north):
            pairs.append((side(place), side(half + place)))
        return pairs

    def gather(k, level, pairs):
        tiles = []
        for tile, (west, east) in zip((tile_south, tile_own, tile_north), pairs):
            side = halo(k, level, west, east)
            if tile is tile_own:
                if k == C:
                    side = jnp.where(lanes == SLOT, turned(rims[1], SLOT - level), side)
                if k in (C, ED, EW):
                    lane_at = {C: 0, ED: 1, EW: 2}[k] * levels + level
                    moved = turned(rims[0], 127 - SLOT - lane_at)
                    side = jnp.where(lanes == 127 - SLOT, moved, side)
            tiles.append(jnp.concatenate([tile(k, level), side], axis=1))
        return jnp.concatenate(tiles, axis=0)

    def rows_of(ref, level, first):
        parts = [ref[level, side, first : first + 24] for side in range(2)]
        return jnp.concatenate(parts, axis=1)

    def middle(ref, level):
        return rows_of(ref, level, 8)

    def to_n(ref, level):
        return rows_of(ref, level, 9)

    def to_s(ref, level):
        return rows_of(ref, level, 7)

    def keep(ref, level, value):
        ref[level, 0, 8:32] = value[:, :128]
        ref[level, 1, 8:32] = value[:, 128:]

    def to_e(v):
        return pltpu.roll(v, 255, 1)

    def to_w(v):
        return pltpu.roll(v, 1, 1)

    def up(level):
        return table[0, level] if level < levels - 1 else None

    def down(level):
        return table[0, level - 1] if level > 0 else None

    def pair(level):
        parts = [u for u in (up(level), down(level)) if u is not None]
        return sum(parts[1:], parts[0])

    def with_levels(total, level, below, above):
        if above is not None:
            total = total - up(level) * above
        if below is not None:
            total = total - down(level) * below
        return total

    def forward_sum(field, level, v, below, above):
        total = up_e[level] * to_e(v) - low_w[level] * to_w(v)
        rows_n = middle(up_n, level) * to_n(field, level)
        total = total + (rows_n - to_s(low_n, level) * to_s(field, level))
        return with_levels(total, level, below, above)

    def adjoint_sum(field, level, v, below, above):
        total = up_w[level] * to_w(v) - low_e[level] * to_e(v)
        rows_s = to_s(up_n, level) * to_s(field, level)
        total = total + (rows_s - middle(low_n, level) * to_n(field, level))
        return with_levels(total, level, below, above)

    def sweep(field, body):
        below, here = None, middle(field, 0)
        for level in range(levels):
            above = middle(field, level + 1) if level + 1 < levels else None
            body(field, level, here, below, above)
            below, here = here, above

    blank = jnp.zeros((8, 128), jnp.float32)
    for level in range(levels):
        for ref in (check, d, x, d_a, mu, up_n, low_n, north):
            faces = any(ref is face for face in (up_n, low_n, north))
            for side in (1,) if faces or ref is check else (0, 1):
                ref[level, side, 0:8] = blank
                if not faces:
                    ref[level, side, 32:40] = blank

    for level in range(levels):
        pairs = strips(level)
        ed = gather(ED, level, pairs)
        ew = gather(EW, level, pairs) * 0.5
        nd = gather(ND, level, pairs)
        nw = gather(NW, level, pairs) * 0.5
        far_nd = far_south(levels + level)
        far_nw = far_south(2 * levels + level) * 0.5
        e_low, e_up, n_low, n_up = ew + ed, ew - ed, nw + nd, nw - nd
        keep(up_n, level, n_up)
        keep(low_n, level, n_low)
        keep(north, level, nd)
        up_n[level, 0, 7:8] = far_nw - far_nd
        low_n[level, 0, 7:8] = far_nw + far_nd
        north[level, 0, 7:8] = far_nd
        w_low, w_up = to_w(e_low), to_w(e_up)
        up_e[level] = e_up
        low_e[level] = e_low
        up_w[level] = w_up
        low_w[level] = w_low
        center = (e_low - w_up) + (n_low - to_s(up_n, level)) + pair(level)
        a_c[level] = center
        base = ed + to_w(ed) + nd + to_s(north, level) + (1.0 + pair(level))
        diag[level] = base
        keep(check, level, gather(C, level, pairs))
        check[level, 0, 7:8] = far_south(level)
        check[level, 0, 32:33] = far_north(level)
        force[level] = gather(S, level, pairs) * cos_ref[...]
        tangent = jnp.tanh(gather(TR, level, pairs))
        local = table[1, level] * (1.0 - tangent * tangent)
        weight_a = RELAXATION / (base + local)
        af = gather(AF, level, pairs)
        diagonal = 1.0 + center + local
        aq_a[level] = diagonal
        wt_a[level] = weight_a
        ctr_a[level] = 1.0 - weight_a * diagonal
        start = weight_a * af
        g_a[level] = start
        keep(d_a, level, start)

    def newton(level, resid, tangent):
        local = table[1, level] * (1.0 - tangent * tangent)
        w = RELAXATION / (diag[level] + local)
        wt[level] = w
        ctr[level] = 1.0 - w * (1.0 + a_c[level] + local)
        start = -(w * resid)
        g[level] = start
        keep(d, level, start)

    def first_resid(field, level, v, below, above):
        tangent = jnp.tanh(v)
        total = forward_sum(field, level, v, below, above)
        resid = total + a_c[level] * v + table[1, level] * tangent - force[level]
        newton(level, resid, tangent)

    def forward_lin(field, level, v, below, above):
        total = forward_sum(field, level, v, below, above)
        keep(field, level, g[level] + ctr[level] * v - wt[level] * total)

    def adjoint_lin(field, level, v, below, above):
        total = adjoint_sum(field, level, v, below, above)
        keep(field, level, g_a[level] + ctr_a[level] * v - wt_a[level] * total)

    def relax(field, body):
        def step(_, carry):
            sweep(field, body)
            return carry

        lax.fori_loop(0, 3, step, 0)

    sweep(check, first_resid)
    relax(d, forward_lin)
    relax(d_a, adjoint_lin)
    for level in range(levels):
        keep(x, level, middle(check, level) + middle(d, level))
        keep(mu, level, middle(d_a, level))

    def second_resid(field, level, v, below, above):
        tangent = jnp.tanh(v)
        total = forward_sum(field, level, v, below, above)
        moved = v - middle(check, level)
        resid = moved + total + a_c[level] * v + table[1, level] * tangent - force[level]
        newton(level, resid, tangent)

    def adjoint_resid(field, level, v, below, above):
        total = adjoint_sum(field, level, v, below, above)
        start = g_a[level] - wt_a[level] * (total + aq_a[level] * v)
        g_a[level] = start
        keep(d_a, level, start)

    sweep(x, second_resid)
    relax(d, forward_lin)
    sweep(mu, adjoint_resid)
    relax(d_a, adjoint_lin)
    for level in range(levels):
        final = middle(x, level) + middle(d, level)
        keep(x, level, final)
        state = final[8:16, :128]
        out_state[level] = state
        multiplier = mu[level, 0, 16:24] + d_a[level, 0, 16:24]
        out_adjoint[level] = multiplier + weight[level] * (state - observations[level])

    def final_resid(field, level, v, below, above):
        total = forward_sum(field, level, v, below, above)
        moved = v - middle(check, level)
        resid = moved + total + a_c[level] * v + table[1, level] * jnp.tanh(v) - force[level]
        out_resid[level] = resid[8:16, :128]

    sweep(x, final_resid)


def vmem(count):
    return [pl.BlockSpec(memory_space=pltpu.VMEM) for _ in range(count)]


def swap(array, axis, start, step, periodic):
    size = lax.axis_size(axis)
    pairs = []
    for low in range(size):
        high = low + step
        if (low - start) % (2 * step) < step and (periodic or high < size):
            pairs += [(low, high % size), (high % size, low)]
    return lax.ppermute(array, axis, pairs)


def compute(
    checkpoint,
    trajectory,
    adjoint_forcing,
    east_diffusion,
    north_diffusion,
    east_wind,
    north_wind,
    level_diffusion,
    damping,
    source,
    observations,
    observation_weight,
    step_index,
):
    levels, lat_rows, lon_cols = checkpoint.shape
    size_x = lax.axis_size("gx")
    size_y = lax.axis_size("gy")
    lane = jnp.arange(256, dtype=jnp.int32)
    column = lax.axis_index("gx") * lon_cols + lane - jnp.where(lane >= 192, 256, 0)
    column = jnp.remainder(column, lon_cols * size_x).astype(jnp.float32)
    phase = (
        2.0 * math.pi * column / (lon_cols * size_x)
        - 2.0 * math.pi * step_index[0].astype(jnp.float32) / DAY_STEPS
    )
    wave = jnp.cos(phase)[None, :]
    index_x, index_y = lax.axis_index("gx"), lax.axis_index("gy")
    place_x = index_x.astype(jnp.int32)[None]
    place_y = index_y.astype(jnp.int32)[None]
    tile = (levels, lat_rows, lon_cols)
    f32 = jnp.float32
    smem = pl.BlockSpec(memory_space=pltpu.SMEM)
    strip = (levels // 2 + 1, lat_rows, lon_cols)
    block, block_f, strip_odd, strip_even = pl.pallas_call(
        functools.partial(pack_kernel, size_y),
        in_specs=[smem, smem] + vmem(8),
        out_specs=vmem(4),
        out_shape=[
            pltpu.VMEM((FIELDS,) + tile, f32),
            pltpu.VMEM((FORWARD,) + tile, f32),
            pltpu.VMEM(strip, f32),
            pltpu.VMEM(strip, f32),
        ],
    )(
        place_x,
        place_y,
        checkpoint,
        source,
        east_diffusion,
        east_wind,
        north_diffusion,
        north_wind,
        trajectory,
        adjoint_forcing,
    )
    from_odd = swap(block_f, "gy", 1, 1, False)
    from_even = swap(block, "gy", 0, 1, False)
    lon_odd = swap(strip_odd, "gx", 1, 1, True)
    lon_even = swap(strip_even, "gx", 0, 1, True)
    corner_shape = (levels + 3 * levels // 8, lat_rows, lon_cols)
    small = pltpu.CompilerParams(vmem_limit_bytes=4 * 1024 * 1024)
    corners, rims, parity = pl.pallas_call(
        corner_odd_kernel,
        in_specs=[smem, smem] + vmem(4),
        out_specs=vmem(3),
        out_shape=[
            pltpu.VMEM((corner_shape[0] + 2 * levels,) + corner_shape[1:], f32),
            pltpu.VMEM((2, lat_rows, lon_cols), f32),
            pltpu.VMEM((lat_rows, lon_cols), f32),
        ],
        compiler_params=small,
    )(place_x, place_y, lon_odd, lon_even, from_even, block)
    corner_odd = swap(corners, "gy", 1, 1, False)
    corners_b, table = pl.pallas_call(
        corner_even_kernel,
        in_specs=[smem] * 3 + vmem(2),
        out_specs=[vmem(1)[0], smem],
        out_shape=[pltpu.VMEM(corner_shape, f32), pltpu.SMEM((2, levels), f32)],
        compiler_params=small,
    )(place_y, level_diffusion, damping, corners, from_odd)
    corner_even = swap(corners_b, "gy", 0, 1, False)
    scratch = [pltpu.VMEM((levels, 2, 40, 128), f32) for _ in range(8)]
    scratch += [pltpu.VMEM((levels, 24, 256), f32) for _ in range(14)]
    return tuple(
        pl.pallas_call(
            solve_kernel,
            in_specs=[smem] + vmem(11),
            out_specs=vmem(3),
            out_shape=[jax.ShapeDtypeStruct(tile, f32)] * 3,
            scratch_shapes=scratch,
            compiler_params=pltpu.CompilerParams(vmem_limit_bytes=20 * 1024 * 1024),
        )(
            table,
            wave,
            parity,
            block,
            from_odd,
            from_even,
            corners,
            corner_odd,
            corner_even,
            rims,
            observations,
            observation_weight,
        )
    )


def solution(mesh):
    spread = P(None, "gy", "gx")
    in_specs = (spread,) * 7 + (P(), P()) + (spread,) * 3 + (P(),)
    return jax.shard_map(
        compute, mesh=mesh, in_specs=in_specs, out_specs=(spread,) * 3, check_vma=False
    )
```

```python
import functools
import math

import jax
import jax.numpy as jnp
from jax import lax
from jax.experimental import pallas as pl
from jax.experimental.pallas import tpu as pltpu
from jax.sharding import PartitionSpec as P

DAY_STEPS = 96
RELAXATION = 0.7
SLOT = 8
FIELDS = 8
FORWARD = 6
C, S, ED, EW, ND, NW, TR, AF = range(8)


def lane_ids():
    return lax.broadcasted_iota(jnp.int32, (8, 128), 1)


def turned(value, shift):
    return value if shift % 128 == 0 else pltpu.roll(value, shift % 128, 1)


def pack_kernel(size_y, x_ref, y_ref, level_ref, damp_ref, *refs):
    fields = refs[:FIELDS]
    block, block_f, strip_odd, strip_even, table = refs[FIELDS:]
    for level in range(fields[0].shape[0]):
        table[0, level] = level_ref[level]
        table[1, level] = damp_ref[level]
    odd_x, last = x_ref[0] % 2 == 1, y_ref[0] == size_y - 1
    levels = fields[0].shape[0]
    half = levels // 2
    lanes = lane_ids()
    row = lax.broadcasted_iota(jnp.int32, (8, 128), 0)
    closed = jnp.where((row == 7) & last, 0.0, 1.0)
    rim_east = jnp.zeros((8, 128), jnp.float32)
    rim_west = jnp.zeros((8, 128), jnp.float32)
    for place in range(half):
        east = jnp.zeros((8, 128), jnp.float32)
        west = jnp.zeros((8, 128), jnp.float32)
        for level in (place, place + half):
            for k in range(FIELDS):
                value = fields[k][level]
                if k in (ND, NW):
                    value = value * closed
                block[k, level] = value
                if k < FORWARD:
                    block_f[k, level] = value
                base = SLOT * k + (64 if level >= half else 0)
                slot = (lanes >= base) & (lanes < base + SLOT)
                east = jnp.where(slot, turned(value, base + SLOT), east)
                west = jnp.where(slot, turned(value, base), west)
                if k == C:
                    rim_west = jnp.where(lanes == level, turned(value, level - SLOT), rim_west)
                if k in (C, ED, EW):
                    lane_at = {C: 0, ED: 1, EW: 2}[k] * levels + level
                    moved = turned(value, lane_at - (127 - SLOT))
                    rim_east = jnp.where(lanes == lane_at, moved, rim_east)
        strip_odd[place] = jnp.where(odd_x, east, west)
        strip_even[place] = jnp.where(odd_x, west, east)
    strip_odd[half] = jnp.where(odd_x, rim_east, rim_west)
    strip_even[half] = jnp.where(odd_x, rim_west, rim_east)


def relay(odd_y, high_when_odd, block, corners):
    levels = block.shape[1]
    for row in range(3 * levels):
        value = block[(C, ND, NW)[row // levels], row % levels]
        high, low = value[7:8], value[0:1]
        line = jnp.where(odd_y, high, low) if high_when_odd else jnp.where(odd_y, low, high)
        at = row % 8
        corners[levels + row // 8, at : at + 1] = line


def corner_odd_kernel(x_ref, y_ref, from_odd, from_even, block_even, block, corners, rims, parity):
    half = from_odd.shape[0] - 1
    odd_x = x_ref[0] % 2 == 1
    for place in range(half):
        corners[place] = jnp.where(odd_x, from_even[place], from_odd[place])
        corners[half + place] = jnp.where(odd_x, from_odd[place], from_even[place])
    parity[...] = jnp.where(y_ref[0] % 2 == 1, 1.0, jnp.zeros((8, 128), jnp.float32))
    rims[0] = jnp.where(odd_x, from_even[half], from_odd[half])
    rims[1] = jnp.where(odd_x, from_odd[half], from_even[half])
    relay(y_ref[0] % 2 == 1, True, block_even, corners)
    levels = block.shape[1]
    base = levels + 3 * levels // 8
    for k in range(FORWARD, FIELDS):
        for level in range(levels):
            corners[base + (k - FORWARD) * levels + level] = block[k, level]


def corner_even_kernel(y_ref, corner_own, block_odd, corners):
    for place in range(block_odd.shape[1]):
        corners[place] = corner_own[place]
    relay(y_ref[0] % 2 == 1, False, block_odd, corners)


def solve_kernel(
    table,
    cos_ref,
    parity,
    own,
    from_odd,
    from_even,
    corner_own,
    corner_odd,
    corner_even,
    rims,
    observations,
    weight,
    out_state,
    out_resid,
    out_adjoint,
    check,
    d,
    x,
    d_a,
    mu,
    up_n,
    low_n,
    north,
    force,
    a_c,
    diag,
    up_e,
    low_w,
    low_e,
    up_w,
    wt,
    ctr,
    g,
    aq_a,
    wt_a,
    ctr_a,
    g_a,
):
    levels = check.shape[0]
    lanes = lane_ids()

    half = levels // 2
    odd_y = parity[...] > 0.5

    def odd_tile(k, at):
        if k < FORWARD:
            return from_odd[k, at]
        return corner_odd[levels + 3 * levels // 8 + (k - FORWARD) * levels + at]

    def tile_south(k, at):
        return jnp.where(odd_y, from_even[k, at], odd_tile(k, at))

    def tile_north(k, at):
        return jnp.where(odd_y, odd_tile(k, at), from_even[k, at])

    def tile_own(k, at):
        return own[k, at]

    def side_south(at):
        return jnp.where(odd_y, corner_even[at], corner_odd[at])

    def side_north(at):
        return jnp.where(odd_y, corner_odd[at], corner_even[at])

    def side_own(at):
        return corner_own[at]

    def far_south(at):
        tile, row = levels + at // 8, at % 8
        return side_south(tile)[row : row + 1]

    def far_north(at):
        tile, row = levels + at // 8, at % 8
        return side_north(tile)[row : row + 1]

    def halo(k, level, west, east):
        base = SLOT * k + (64 if level >= half else 0)
        left = turned(west, 128 - SLOT - base)
        right = turned(east, -base)
        return jnp.where(lanes < SLOT, right, jnp.where(lanes >= 128 - SLOT, left, 0.0))

    def strips(level):
        place = level % half
        pairs = []
        for side in (side_south, side_own, side_north):
            pairs.append((side(place), side(half + place)))
        return pairs

    def gather(k, level, pairs):
        tiles = []
        for tile, (west, east) in zip((tile_south, tile_own, tile_north), pairs):
            side = halo(k, level, west, east)
            if tile is tile_own:
                if k == C:
                    side = jnp.where(lanes == SLOT, turned(rims[1], SLOT - level), side)
                if k in (C, ED, EW):
                    lane_at = {C: 0, ED: 1, EW: 2}[k] * levels + level
                    moved = turned(rims[0], 127 - SLOT - lane_at)
                    side = jnp.where(lanes == 127 - SLOT, moved, side)
            tiles.append(jnp.concatenate([tile(k, level), side], axis=1))
        return jnp.concatenate(tiles, axis=0)

    def rows_of(ref, level, first):
        parts = [ref[level, side, first : first + 24] for side in range(2)]
        return jnp.concatenate(parts, axis=1)

    def middle(ref, level):
        return rows_of(ref, level, 8)

    def to_n(ref, level):
        return rows_of(ref, level, 9)

    def to_s(ref, level):
        return rows_of(ref, level, 7)

    def keep(ref, level, value):
        ref[level, 0, 8:32] = value[:, :128]
        ref[level, 1, 8:32] = value[:, 128:]

    def to_e(v):
        return pltpu.roll(v, 255, 1)

    def to_w(v):
        return pltpu.roll(v, 1, 1)

    def up(level):
        return table[0, level] if level < levels - 1 else None

    def down(level):
        return table[0, level - 1] if level > 0 else None

    def pair(level):
        parts = [u for u in (up(level), down(level)) if u is not None]
        return sum(parts[1:], parts[0])

    def with_levels(total, level, below, above):
        if above is not None:
            total = total - up(level) * above
        if below is not None:
            total = total - down(level) * below
        return total

    def forward_sum(field, level, v, below, above):
        total = up_e[level] * to_e(v) - low_w[level] * to_w(v)
        rows_n = middle(up_n, level) * to_n(field, level)
        total = total + (rows_n - to_s(low_n, level) * to_s(field, level))
        return with_levels(total, level, below, above)

    def adjoint_sum(field, level, v, below, above):
        total = up_w[level] * to_w(v) - low_e[level] * to_e(v)
        rows_s = to_s(up_n, level) * to_s(field, level)
        total = total + (rows_s - middle(low_n, level) * to_n(field, level))
        return with_levels(total, level, below, above)

    def sweep(field, body):
        below, here = None, middle(field, 0)
        for level in range(levels):
            above = middle(field, level + 1) if level + 1 < levels else None
            body(field, level, here, below, above)
            below, here = here, above

    blank = jnp.zeros((8, 128), jnp.float32)
    for level in range(levels):
        for ref in (check, d, x, d_a, mu, up_n, low_n, north):
            faces = any(ref is face for face in (up_n, low_n, north))
            for side in (1,) if faces or ref is check else (0, 1):
                ref[level, side, 0:8] = blank
                if not faces:
                    ref[level, side, 32:40] = blank

    for level in range(levels):
        pairs = strips(level)
        ed = gather(ED, level, pairs)
        ew = gather(EW, level, pairs) * 0.5
        nd = gather(ND, level, pairs)
        nw = gather(NW, level, pairs) * 0.5
        far_nd = far_south(levels + level)
        far_nw = far_south(2 * levels + level) * 0.5
        e_low, e_up, n_low, n_up = ew + ed, ew - ed, nw + nd, nw - nd
        keep(up_n, level, n_up)
        keep(low_n, level, n_low)
        keep(north, level, nd)
        up_n[level, 0, 7:8] = far_nw - far_nd
        low_n[level, 0, 7:8] = far_nw + far_nd
        north[level, 0, 7:8] = far_nd
        w_low, w_up = to_w(e_low), to_w(e_up)
        up_e[level] = e_up
        low_e[level] = e_low
        up_w[level] = w_up
        low_w[level] = w_low
        center = (e_low - w_up) + (n_low - to_s(up_n, level)) + pair(level)
        a_c[level] = center
        base = ed + to_w(ed) + nd + to_s(north, level) + (1.0 + pair(level))
        diag[level] = base
        keep(check, level, gather(C, level, pairs))
        check[level, 0, 7:8] = far_south(level)
        check[level, 0, 32:33] = far_north(level)
        force[level] = gather(S, level, pairs) * cos_ref[...]
        tangent = jnp.tanh(gather(TR, level, pairs))
        local = table[1, level] * (1.0 - tangent * tangent)
        weight_a = RELAXATION / (base + local)
        af = gather(AF, level, pairs)
        diagonal = 1.0 + center + local
        aq_a[level] = diagonal
        wt_a[level] = weight_a
        ctr_a[level] = 1.0 - weight_a * diagonal
        start = weight_a * af
        g_a[level] = start
        keep(d_a, level, start)

    def newton(level, resid, tangent):
        local = table[1, level] * (1.0 - tangent * tangent)
        w = RELAXATION / (diag[level] + local)
        wt[level] = w
        ctr[level] = 1.0 - w * (1.0 + a_c[level] + local)
        start = -(w * resid)
        g[level] = start
        keep(d, level, start)

    def first_resid(field, level, v, below, above):
        tangent = jnp.tanh(v)
        total = forward_sum(field, level, v, below, above)
        resid = total + a_c[level] * v + table[1, level] * tangent - force[level]
        newton(level, resid, tangent)

    def forward_lin(field, level, v, below, above):
        total = forward_sum(field, level, v, below, above)
        keep(field, level, g[level] + ctr[level] * v - wt[level] * total)

    def adjoint_lin(field, level, v, below, above):
        total = adjoint_sum(field, level, v, below, above)
        keep(field, level, g_a[level] + ctr_a[level] * v - wt_a[level] * total)

    def relax(field, body):
        def step(_, carry):
            sweep(field, body)
            return carry

        lax.fori_loop(0, 3, step, 0)

    sweep(check, first_resid)
    relax(d, forward_lin)
    relax(d_a, adjoint_lin)
    for level in range(levels):
        keep(x, level, middle(check, level) + middle(d, level))
        keep(mu, level, middle(d_a, level))

    def second_resid(field, level, v, below, above):
        tangent = jnp.tanh(v)
        total = forward_sum(field, level, v, below, above)
        moved = v - middle(check, level)
        resid = moved + total + a_c[level] * v + table[1, level] * tangent - force[level]
        newton(level, resid, tangent)

    def adjoint_resid(field, level, v, below, above):
        total = adjoint_sum(field, level, v, below, above)
        start = g_a[level] - wt_a[level] * (total + aq_a[level] * v)
        g_a[level] = start
        keep(d_a, level, start)

    sweep(x, second_resid)
    relax(d, forward_lin)
    sweep(mu, adjoint_resid)
    relax(d_a, adjoint_lin)
    for level in range(levels):
        final = middle(x, level) + middle(d, level)
        keep(x, level, final)
        state = final[8:16, :128]
        out_state[level] = state
        multiplier = mu[level, 0, 16:24] + d_a[level, 0, 16:24]
        out_adjoint[level] = multiplier + weight[level] * (state - observations[level])

    def final_resid(field, level, v, below, above):
        total = forward_sum(field, level, v, below, above)
        moved = v - middle(check, level)
        resid = moved + total + a_c[level] * v + table[1, level] * jnp.tanh(v) - force[level]
        out_resid[level] = resid[8:16, :128]

    sweep(x, final_resid)


def vmem(count):
    return [pl.BlockSpec(memory_space=pltpu.VMEM) for _ in range(count)]


def swap(array, axis, start, step, periodic):
    size = lax.axis_size(axis)
    pairs = []
    for low in range(size):
        high = low + step
        if (low - start) % (2 * step) < step and (periodic or high < size):
            pairs += [(low, high % size), (high % size, low)]
    return lax.ppermute(array, axis, pairs)


def compute(
    checkpoint,
    trajectory,
    adjoint_forcing,
    east_diffusion,
    north_diffusion,
    east_wind,
    north_wind,
    level_diffusion,
    damping,
    source,
    observations,
    observation_weight,
    step_index,
):
    levels, lat_rows, lon_cols = checkpoint.shape
    size_x = lax.axis_size("gx")
    size_y = lax.axis_size("gy")
    lane = jnp.arange(256, dtype=jnp.int32)
    column = lax.axis_index("gx") * lon_cols + lane - jnp.where(lane >= 192, 256, 0)
    column = jnp.remainder(column, lon_cols * size_x).astype(jnp.float32)
    phase = (
        2.0 * math.pi * column / (lon_cols * size_x)
        - 2.0 * math.pi * step_index[0].astype(jnp.float32) / DAY_STEPS
    )
    wave = jnp.cos(phase)[None, :]
    index_x, index_y = lax.axis_index("gx"), lax.axis_index("gy")
    place_x = index_x.astype(jnp.int32)[None]
    place_y = index_y.astype(jnp.int32)[None]
    tile = (levels, lat_rows, lon_cols)
    f32 = jnp.float32
    smem = pl.BlockSpec(memory_space=pltpu.SMEM)
    strip = (levels // 2 + 1, lat_rows, lon_cols)
    block, block_f, strip_odd, strip_even, table = pl.pallas_call(
        functools.partial(pack_kernel, size_y),
        in_specs=[smem] * 4 + vmem(8),
        out_specs=vmem(4) + [smem],
        out_shape=[
            pltpu.VMEM((FIELDS,) + tile, f32),
            pltpu.VMEM((FORWARD,) + tile, f32),
            pltpu.VMEM(strip, f32),
            pltpu.VMEM(strip, f32),
            pltpu.SMEM((2, levels), f32),
        ],
    )(
        place_x,
        place_y,
        level_diffusion,
        damping,
        checkpoint,
        source,
        east_diffusion,
        east_wind,
        north_diffusion,
        north_wind,
        trajectory,
        adjoint_forcing,
    )
    from_odd = swap(block_f, "gy", 1, 1, False)
    from_even = swap(block, "gy", 0, 1, False)
    lon_odd = swap(strip_odd, "gx", 1, 1, True)
    lon_even = swap(strip_even, "gx", 0, 1, True)
    corner_shape = (levels + 3 * levels // 8, lat_rows, lon_cols)
    small = pltpu.CompilerParams(vmem_limit_bytes=4 * 1024 * 1024)
    corners, rims, parity = pl.pallas_call(
        corner_odd_kernel,
        in_specs=[smem, smem] + vmem(4),
        out_specs=vmem(3),
        out_shape=[
            pltpu.VMEM((corner_shape[0] + 2 * levels,) + corner_shape[1:], f32),
            pltpu.VMEM((2, lat_rows, lon_cols), f32),
            pltpu.VMEM((lat_rows, lon_cols), f32),
        ],
        compiler_params=small,
    )(place_x, place_y, lon_odd, lon_even, from_even, block)
    corner_odd = swap(corners, "gy", 1, 1, False)
    corners_b = pl.pallas_call(
        corner_even_kernel,
        in_specs=[smem] + vmem(2),
        out_specs=vmem(1)[0],
        out_shape=pltpu.VMEM(corner_shape, f32),
        compiler_params=small,
    )(place_y, corners, from_odd)
    corner_even = swap(corners_b, "gy", 0, 1, False)
    scratch = [pltpu.VMEM((levels, 2, 40, 128), f32) for _ in range(8)]
    scratch += [pltpu.VMEM((levels, 24, 256), f32) for _ in range(14)]
    return tuple(
        pl.pallas_call(
            solve_kernel,
            in_specs=[smem] + vmem(11),
            out_specs=vmem(3),
            out_shape=[jax.ShapeDtypeStruct(tile, f32)] * 3,
            scratch_shapes=scratch,
            compiler_params=pltpu.CompilerParams(vmem_limit_bytes=20 * 1024 * 1024),
        )(
            table,
            wave,
            parity,
            block,
            from_odd,
            from_even,
            corners,
            corner_odd,
            corner_even,
            rims,
            observations,
            observation_weight,
        )
    )


def solution(mesh):
    spread = P(None, "gy", "gx")
    in_specs = (spread,) * 7 + (P(), P()) + (spread,) * 3 + (P(),)
    return jax.shard_map(
        compute, mesh=mesh, in_specs=in_specs, out_specs=(spread,) * 3, check_vma=False
    )
```
